32 devices in a mesh: data: 2 (over x), dap2: 4 (over z), dap: 4 (over y, core).
Axes of the slice: x: 2, y: 2, z: 4, core: 2. Of those that a mesh axis runs over, the one named last changes fastest.
Arguments:
- pair_act: bfloat16 [1280, 640, 128], P(('data', 'dap'), 'dap2'), parts along dimension 0
- pair_mask: int32 [1280, 640], P(('data', 'dap'), 'dap2'), parts along dimension 0
- in_gamma: float32 [2, 2, 128], replicated
- in_beta: float32 [2, 2, 128], replicated
- w_proj: bfloat16 [2, 2, 128, 512], replicated
- w_gate: bfloat16 [2, 2, 128, 128], replicated
- out_gamma: float32 [2, 2, 128], replicated
- out_beta: float32 [2, 2, 128], replicated
- w_out: bfloat16 [2, 2, 128, 128], replicated
Outputs:
- output: bfloat16 [1280, 640, 128], P(('data', 'dap'), 'dap2'), parts along dimension 0
There are 2 independent parts. The reference program is written for one: setup_inputs(seed, part) draws one part's arguments, and reference() takes and returns one part's arrays. A program takes and returns all parts, laid end to end along the dimension named above; an argument that names none is the same for every part.
All inputs are finite; a program needn't handle non-finite values.
Results may differ from the reference program's by a relative error of at most 0.0112834.
Values are sent between devices in bfloat16 or wider.
A program may use at most 1 GiB of HBM per device.

```python
import jax
import jax.numpy as jnp
from jax import lax

RESIDUES = 640
PAIR_DIM = 128
TRI_DIM = 128
BLOCKS = 2
NORM_EPS = 1e-5


def setup_inputs(seed: int = 0, part: int = 0) -> dict:
    key_list = jax.random.split(jax.random.key(seed), 9)
    pair_key = jax.random.fold_in(key_list[0], part)
    mask_key = jax.random.fold_in(key_list[1], part)
    pair_act = jax.random.normal(pair_key, (RESIDUES, RESIDUES, PAIR_DIM), jnp.float32).astype(jnp.bfloat16)
    row_valid = (jax.random.randint(mask_key, (RESIDUES,), 0, 16) != 0).astype(jnp.int32)
    pair_mask = row_valid[:, None] * row_valid[None, :]
    stack_shape = (BLOCKS, 2)
    in_gamma = 1.0 + 0.3 * jax.random.normal(key_list[2], stack_shape + (PAIR_DIM,), jnp.float32)
    in_beta = 0.3 * jax.random.normal(key_list[3], stack_shape + (PAIR_DIM,), jnp.float32)
    w_proj = (jax.random.normal(key_list[4], stack_shape + (PAIR_DIM, 4 * TRI_DIM), jnp.float32) * PAIR_DIM ** -0.5).astype(jnp.bfloat16)
    w_gate = (jax.random.normal(key_list[5], stack_shape + (PAIR_DIM, PAIR_DIM), jnp.float32) * PAIR_DIM ** -0.5).astype(jnp.bfloat16)
    out_gamma = 1.0 + 0.3 * jax.random.normal(key_list[6], stack_shape + (TRI_DIM,), jnp.float32)
    out_beta = 0.3 * jax.random.normal(key_list[7], stack_shape + (TRI_DIM,), jnp.float32)
    w_out = (jax.random.normal(key_list[8], stack_shape + (TRI_DIM, PAIR_DIM), jnp.float32) * TRI_DIM ** -0.5).astype(jnp.bfloat16)
    return {'pair_act': pair_act, 'pair_mask': pair_mask, 'in_gamma': in_gamma, 'in_beta': in_beta, 'w_proj': w_proj, 'w_gate': w_gate, 'out_gamma': out_gamma, 'out_beta': out_beta, 'w_out': w_out}


def layer_norm(values, gamma, beta):
    centered = values - jnp.mean(values, axis=-1, keepdims=True)
    variance = jnp.mean(centered * centered, axis=-1, keepdims=True)
    return centered * lax.rsqrt(variance + NORM_EPS) * gamma + beta


def project_row(pair_row, mask_row, gamma_in, beta_in, w_proj):
    normed = layer_norm(pair_row.astype(jnp.float32), gamma_in, beta_in).astype(jnp.bfloat16)
    projected = jnp.dot(normed, w_proj, preferred_element_type=jnp.float32)
    mask_col = mask_row.astype(jnp.float32)[:, None]
    left = mask_col * jax.nn.sigmoid(projected[:, TRI_DIM:2 * TRI_DIM]) * projected[:, :TRI_DIM]
    right = mask_col * jax.nn.sigmoid(projected[:, 3 * TRI_DIM:]) * projected[:, 2 * TRI_DIM:3 * TRI_DIM]
    return left.astype(jnp.bfloat16), right.astype(jnp.bfloat16)


def finish_row(pair_row, tri_row, gamma_in, beta_in, w_gate, gamma_out, beta_out, w_out):
    normed = layer_norm(pair_row.astype(jnp.float32), gamma_in, beta_in).astype(jnp.bfloat16)
    gate = jax.nn.sigmoid(jnp.dot(normed, w_gate, preferred_element_type=jnp.float32))
    tri_normed = layer_norm(tri_row.astype(jnp.float32), gamma_out, beta_out).astype(jnp.bfloat16)
    update = jnp.dot(tri_normed, w_out, preferred_element_type=jnp.float32)
    return (pair_row.astype(jnp.float32) + gate * update).astype(jnp.bfloat16)


def triangle_update(pair_act, pair_mask, params, incoming):
    gamma_in, beta_in, w_proj, w_gate, gamma_out, beta_out, w_out = params
    left, right = lax.map(lambda rows: project_row(rows[0], rows[1], gamma_in, beta_in, w_proj), (pair_act, pair_mask))
    einsum_form = 'kic,kjc->ijc' if incoming else 'ikc,jkc->ijc'
    tri_out = jnp.einsum(einsum_form, left.astype(jnp.float32), right.astype(jnp.float32)).astype(jnp.bfloat16)
    return lax.map(lambda rows: finish_row(rows[0], rows[1], gamma_in, beta_in, w_gate, gamma_out, beta_out, w_out), (pair_act, tri_out))


def reference(pair_act, pair_mask, in_gamma, in_beta, w_proj, w_gate, out_gamma, out_beta, w_out):
    def block_step(carry, params):
        outgoing = tuple(leaf[0] for leaf in params)
        incoming = tuple(leaf[1] for leaf in params)
        carry = triangle_update(carry, pair_mask, outgoing, False)
        carry = triangle_update(carry, pair_mask, incoming, True)
        return carry, None
    result, _ = lax.scan(block_step, pair_act, (in_gamma, in_beta, w_proj, w_gate, out_gamma, out_beta, w_out))
    return result
```

```python
import functools

import jax
import jax.numpy as jnp
from jax import lax
from jax.experimental import pallas as pl
from jax.experimental.pallas import tpu as pltpu
from jax.sharding import PartitionSpec as P

NORM_EPS = 1e-5
F32 = jnp.float32
BF16 = jnp.bfloat16
MESH = pl.DeviceIdType.MESH
ND = 16
CPD = 8
B = 160
GR = 4
RR = 40
SL = 8
STEPS = RR // SL
SWAP = 136


def to_tiles(block):
    rest = block.shape[2:]
    grouped = block.reshape((GR, RR, B) + rest)
    main = grouped[:, :, :128]
    rem = jnp.swapaxes(grouped[:, :, 128:], 0, 1).reshape((1, RR, 128) + rest)
    return jnp.concatenate([main, jnp.swapaxes(rem, 0, 0)], axis=0)


def from_tiles(tiles):
    rest = tiles.shape[3:]
    main = tiles[:GR]
    rem = jnp.swapaxes(tiles[GR].reshape((RR, GR, 32) + rest), 0, 1)
    return jnp.concatenate([main, rem], axis=2).reshape((B, B) + rest)


def sigmoid(v):
    return 0.5 * jnp.tanh(0.5 * v) + 0.5


def norm_lanes(values, gamma, beta):
    centered = values - jnp.mean(values, axis=-1, keepdims=True)
    variance = jnp.mean(centered * centered, axis=-1, keepdims=True)
    return centered * lax.rsqrt(variance + NORM_EPS) * gamma + beta


def my_place():
    row, col = lax.axis_index('dap'), lax.axis_index('dap2')
    return row, col, row * 4 + col


def partner(me, n):
    other = lax.rem(me + n, ND)
    return other, {'dap': other // 4, 'dap2': lax.rem(other, 4)}


def greet(me):
    barrier = pltpu.get_barrier_semaphore()

    def signal(n, carry):
        _, device = partner(me, n)
        pl.semaphore_signal(barrier, inc=1, device_id=device, device_id_type=MESH)
        return carry

    lax.fori_loop(1, ND, signal, 0)
    return barrier


def position_kernel(finish, project, *refs):
    refs = list(refs)
    take = lambda: refs.pop(0)
    z_ref = take()
    if finish:
        t_ref, gin_ref, bin_ref, wg_ref, gout_ref, bout_ref, wo_ref = [take() for _ in range(7)]
    if project:
        mask_ref, gnext_ref, bnext_ref, wp_ref = [take() for _ in range(4)]
    if finish:
        zo_ref = take()
    if project:
        a_in, b_in = take(), take()
    if finish:
        y_buf = take()
    if project:
        sa, sb, out_a, out_b, send_sem, recv_sem = [take() for _ in range(6)]
    s = pl.program_id(0)
    if project:
        row, col, me = my_place()
        barrier = pltpu.get_barrier_semaphore()

        @pl.when(s == 0)
        def _():
            greet(me)

    def group(grp, carry):
        if finish:
            total = jnp.zeros((SL, 128), F32)
            for cb in range(8):
                total += jnp.sum(t_ref[cb * 16:(cb + 1) * 16, grp].astype(F32), axis=0)
            mean = (total * (1.0 / 128))[None]
            total = jnp.zeros((SL, 128), F32)
            for cb in range(8):
                centered = t_ref[cb * 16:(cb + 1) * 16, grp].astype(F32) - mean
                total += jnp.sum(centered * centered, axis=0)
            scale = lax.rsqrt(total * (1.0 / 128) + NORM_EPS)[None]
            for cb in range(8):
                sl = slice(cb * 16, (cb + 1) * 16)
                y = (t_ref[sl, grp].astype(F32) - mean) * scale * gout_ref[sl] + bout_ref[sl]
                y_buf[cb * 128:(cb + 1) * 128, :] = y.reshape(128, 128)

        def tile(r, inner):
            zf = z_ref[grp, r].astype(F32)
            if finish:
                x = norm_lanes(zf, gin_ref[...], bin_ref[...]).astype(BF16)
                gate = sigmoid(jnp.dot(x, wg_ref[...], preferred_element_type=F32))
                y = y_buf[pl.ds(r, 128, stride=SL), :].astype(BF16)
                update = lax.dot_general(y, wo_ref[...], (((0,), (0,)), ((), ())), preferred_element_type=F32)
                znew = (zf + gate * update).astype(BF16)
                zo_ref[grp, r] = znew
                zf = znew.astype(F32)
            if project:
                x = norm_lanes(zf, gnext_ref[...], bnext_ref[...]).astype(BF16)
                q = lax.dot_general(wp_ref[...], x, (((1,), (1,)), ((), ())), preferred_element_type=F32)
                m = mask_ref[grp, pl.ds(r, 1), :]
                base = pl.multiple_of(r * SWAP, 8)
                sa[pl.ds(base, 128), :] = m * sigmoid(q[128:256]) * q[:128]
                sb[pl.ds(base, 128), :] = m * sigmoid(q[384:]) * q[256:384]
            return inner

        lax.fori_loop(0, SL, tile, 0, unroll=2)

        if project:
            def swap(cb, inner):
                for u in range(8):
                    c = cb * 8 + u
                    out_a[s, c, grp] = sa[pl.ds(c, SL, stride=SWAP), :].astype(BF16)
                    out_b[s, c, grp] = sb[pl.ds(c, SL, stride=SWAP), :].astype(BF16)
                return inner

            lax.fori_loop(0, 16, swap, 0)
        return carry

    lax.fori_loop(0, 5, group, 0)

    if project:
        @pl.when(s == 0)
        def _():
            pl.semaphore_wait(barrier, ND - 1)

        rows = pl.ds(pl.multiple_of(s * SL, SL), SL)
        lanes = pl.ds(pl.multiple_of(col * 128, 128), 128)

        def send(n, carry):
            other, device = partner(me, n)
            chans = pl.ds(other * CPD, CPD)
            for k, (src, dst) in enumerate(((out_a, a_in), (out_b, b_in))):
                pltpu.make_async_remote_copy(
                    src_ref=src.at[s, chans], dst_ref=dst.at[:, row, :, rows, lanes],
                    send_sem=send_sem.at[k], recv_sem=recv_sem.at[k],
                    device_id=device, device_id_type=MESH).start()
            return carry

        lax.fori_loop(1, ND, send, 0)
        for k, (src, dst) in enumerate(((out_a, a_in), (out_b, b_in))):
            pltpu.make_async_copy(src.at[s, pl.ds(me * CPD, CPD)], dst.at[:, row, :, rows, lanes], recv_sem.at[k]).start()

        @pl.when(s == STEPS - 1)
        def _():
            for k, (src, dst) in enumerate(((out_a, a_in), (out_b, b_in))):
                pltpu.make_async_copy(dst, dst, recv_sem.at[k]).wait()
                sent = src.at[:, pl.ds(0, 128 - CPD)]
                pltpu.make_async_copy(sent, sent, send_sem.at[k]).wait()


def position_call(z_tiles, finish_args, project_args, collective_id):
    finish, project = finish_args is not None, project_args is not None
    full = lambda arr: pl.BlockSpec(arr.shape, lambda s: (0,) * arr.ndim)
    z_spec = pl.BlockSpec((5, SL, 128, 128), lambda s: (0, s, 0, 0))
    args, specs = [z_tiles], [z_spec]
    outs, out_specs, scratch = [], [], []
    if finish:
        args += list(finish_args)
        specs += [pl.BlockSpec((128, 5, SL, 128), lambda s: (0, 0, s, 0))] + [full(v) for v in finish_args[1:]]
        outs.append(jax.ShapeDtypeStruct(z_tiles.shape, BF16))
        out_specs.append(z_spec)
        scratch.append(pltpu.VMEM((128 * SL, 128), F32))
    if project:
        args += list(project_args)
        specs += [pl.BlockSpec((5, SL, 128), lambda s: (0, s, 0))] + [full(v) for v in project_args[1:]]
        outs += [jax.ShapeDtypeStruct((CPD, 4, 5, RR, 512), BF16)] * 2
        out_specs += [pl.BlockSpec(memory_space=pl.ANY)] * 2
        scratch += [pltpu.VMEM((SWAP * SL, 128), F32)] * 2
        scratch += [pltpu.VMEM((STEPS, 128, 5, SL, 128), BF16)] * 2
        scratch += [pltpu.SemaphoreType.DMA((2,)), pltpu.SemaphoreType.DMA((2,))]
    params = dict(dimension_semantics=('arbitrary',), vmem_limit_bytes=60 * 2 ** 20)
    if project:
        params.update(collective_id=collective_id, has_side_effects=True)
    name = 'position' + ('_finish' if finish else '') + ('_project' if project else '')
    return pl.pallas_call(
        functools.partial(position_kernel, finish, project), name=name, grid=(STEPS,),
        in_specs=specs, out_specs=out_specs, out_shape=outs, scratch_shapes=scratch,
        compiler_params=pltpu.CompilerParams(**params))(*args)


def channel_kernel(incoming, a_ref, b_ref, perm_ref, t_in, amat, bmat, tmat, t_out, send_sem, recv_sem):
    c = pl.program_id(0)
    row, col, me = my_place()
    barrier = pltpu.get_barrier_semaphore()

    @pl.when(c == 0)
    def _():
        greet(me)

    def rem_columns(ref):
        packed = ref[0, :, B:, :].astype(F32).reshape(4 * RR, 512).astype(BF16)
        return jnp.dot(packed, perm_ref[...], preferred_element_type=F32)

    def natural(wide, blk):
        return jnp.concatenate([wide[blk * RR:(blk + 1) * RR, g * 128:(g + 1) * 128] for g in range(GR)], axis=0)

    wide = rem_columns(a_ref)
    for blk in range(4):
        amat[blk * B:(blk + 1) * B, :512] = a_ref[0, blk, :B, :]
        amat[blk * B:(blk + 1) * B, 512:] = natural(wide, blk).astype(BF16)
    wide = rem_columns(b_ref)
    for blk in range(4):
        if incoming:
            bmat[blk * B:(blk + 1) * B, :512] = b_ref[0, blk, :B, :]
            bmat[blk * B:(blk + 1) * B, 512:] = natural(wide, blk).astype(BF16)
        else:
            last = natural(wide, blk).astype(BF16)
            bmat[blk * 128:(blk + 1) * 128, :512] = b_ref[0, blk, :128, :]
            bmat[512 + blk * 32:512 + (blk + 1) * 32, :512] = b_ref[0, blk, 128:B, :]
            bmat[blk * 128:(blk + 1) * 128, 512:] = last[:128]
            bmat[512 + blk * 32:512 + (blk + 1) * 32, 512:] = last[128:]
    contract = 0 if incoming else 1
    tmat[...] = lax.dot_general(amat[...], bmat[...], (((contract,), (contract,)), ((), ())), preferred_element_type=F32)

    def rows_of(blk, lanes):
        if incoming:
            return jnp.concatenate([tmat[blk * 128:(blk + 1) * 128, lanes], tmat[512 + blk * 32:512 + (blk + 1) * 32, lanes]], axis=0)
        return tmat[blk * B:(blk + 1) * B, lanes]

    packed = []
    for blk in range(4):
        for j in range(4):
            t_out[c, blk * 4 + j, :B, :] = rows_of(blk, slice(j * 128, (j + 1) * 128)).astype(BF16)
        rem = rows_of(blk, slice(512, 640))
        packed.append(jnp.concatenate([rem[g * RR:(g + 1) * RR] for g in range(GR)], axis=1))
    wide = jnp.dot(jnp.concatenate(packed, axis=0).astype(BF16), perm_ref[...], preferred_element_type=F32)
    for blk in range(4):
        for j in range(4):
            t_out[c, blk * 4 + j, B:, :] = wide[blk * RR:(blk + 1) * RR, j * 128:(j + 1) * 128].astype(BF16)

    @pl.when(c == 0)
    def _():
        pl.semaphore_wait(barrier, ND - 1)

    def send(n, carry):
        other, device = partner(me, n)
        pltpu.make_async_remote_copy(
            src_ref=t_out.at[c, other], dst_ref=t_in.at[me * CPD + c],
            send_sem=send_sem, recv_sem=recv_sem, device_id=device, device_id_type=MESH).start()
        return carry

    lax.fori_loop(1, ND, send, 0)
    pltpu.make_async_copy(t_out.at[c, me], t_in.at[me * CPD + c], recv_sem).start()

    @pl.when(c == CPD - 1)
    def _():
        pltpu.make_async_copy(t_in, t_in, recv_sem).wait()
        sent = t_out.at[:, pl.ds(0, ND - 1)]
        pltpu.make_async_copy(sent, sent, send_sem).wait()


def channel_call(a_in, b_in, perm, incoming):
    spec = pl.BlockSpec((1, 4, 200, 512), lambda c: (c, 0, 0, 0))
    return pl.pallas_call(
        functools.partial(channel_kernel, incoming), name='channel_in' if incoming else 'channel_out', grid=(CPD,),
        in_specs=[spec, spec, pl.BlockSpec((512, 512), lambda c: (0, 0))],
        out_specs=pl.BlockSpec(memory_space=pl.ANY),
        out_shape=jax.ShapeDtypeStruct((128, 200, 128), BF16),
        scratch_shapes=[
            pltpu.VMEM((640, 640), BF16), pltpu.VMEM((640, 640), BF16), pltpu.VMEM((640, 640), F32),
            pltpu.VMEM((CPD, ND, 200, 128), BF16),
            pltpu.SemaphoreType.DMA, pltpu.SemaphoreType.DMA],
        compiler_params=pltpu.CompilerParams(
            dimension_semantics=('arbitrary',), vmem_limit_bytes=60 * 2 ** 20,
            collective_id=4 if incoming else 3, has_side_effects=True),
    )(a_in.reshape(CPD, 4, 200, 512), b_in.reshape(CPD, 4, 200, 512), perm)


def solution(mesh):
    pair_spec = P(('data', 'dap'), 'dap2', None)
    mask_spec = P(('data', 'dap'), 'dap2')

    def local_fn(pair_act, pair_mask, in_gamma, in_beta, w_proj, w_gate, out_gamma, out_beta, w_out):
        mask = to_tiles(pair_mask.astype(F32))
        z = to_tiles(pair_act)
        src = jnp.arange(512)
        perm = (((src % 128) // 32 * 128 + src // 128 * 32 + src % 32)[:, None] == jnp.arange(512)[None, :]).astype(BF16)
        updates = [(layer, u) for layer in range(in_gamma.shape[0]) for u in range(2)]

        def project_args(at):
            return (mask, in_gamma[at][None], in_beta[at][None], w_proj[at].T)

        def finish_args(at, t):
            wide = lambda v: jnp.broadcast_to(v[at][:, None, None], (128, 1, 128))
            return (t.reshape(128, 5, RR, 128), in_gamma[at][None], in_beta[at][None], w_gate[at], wide(out_gamma), wide(out_beta), w_out[at])

        a_in, b_in = position_call(z, None, project_args(updates[0]), 1)
        for n, at in enumerate(updates):
            t = channel_call(a_in, b_in, perm, at[1] == 1)
            if n + 1 < len(updates):
                z, a_in, b_in = position_call(z, finish_args(at, t), project_args(updates[n + 1]), 2)
            else:
                z, = position_call(z, finish_args(at, t), None, None)
        return from_tiles(z)

    return jax.shard_map(local_fn, mesh=mesh, in_specs=(pair_spec, mask_spec) + (P(),) * 7, out_specs=pair_spec, check_vma=False)
```

```python
import functools

import jax
import jax.numpy as jnp
from jax import lax
from jax.experimental import pallas as pl
from jax.experimental.pallas import tpu as pltpu
from jax.sharding import PartitionSpec as P

NORM_EPS = 1e-5
F32 = jnp.float32
BF16 = jnp.bfloat16
MESH = pl.DeviceIdType.MESH
ND = 16
B = 160
GR = 4
RR = 40
SL = 8
STEPS = RR // SL
UNROLL = 4
SWAP = 136


def to_tiles(block):
    rest = block.shape[2:]
    grouped = block.reshape((GR, RR, B) + rest)
    main = grouped[:, :, :128]
    rem = jnp.swapaxes(grouped[:, :, 128:], 0, 1).reshape((1, RR, 128) + rest)
    return jnp.concatenate([main, rem], axis=0)


def sigmoid(v):
    return 0.5 * jnp.tanh(0.5 * v) + 0.5


def norm_lanes(values, gamma, beta):
    centered = values - jnp.mean(values, axis=-1, keepdims=True)
    variance = jnp.mean(centered * centered, axis=-1, keepdims=True)
    return centered * lax.rsqrt(variance + NORM_EPS) * gamma + beta


def place(team):
    row, col = lax.axis_index('dap'), lax.axis_index('dap2')
    return row * 4 + col if team == ND else row * 2 + lax.rem(col, 2)


def partner(team, n):
    other = lax.rem(place(team) + n, team)
    if team == ND:
        return other, {'dap': other // 4, 'dap2': lax.rem(other, 4)}
    half = lax.axis_index('dap2') // 2
    return other, {'dap': other // 2, 'dap2': half * 2 + lax.rem(other, 2)}


def greet(team):
    barrier = pltpu.get_barrier_semaphore()

    def signal(n, carry):
        _, device = partner(team, n)
        pl.semaphore_signal(barrier, inc=1, device_id=device, device_id_type=MESH)
        return carry

    lax.fori_loop(1, team, signal, 0)


def position_kernel(finish, project, natural_in, *refs):
    refs = list(refs)
    take = lambda: refs.pop(0)
    z_in = take()
    if finish:
        t_ref, gin_ref, bin_ref, wg_ref, gout_ref, bout_ref, wo_ref = [take() for _ in range(7)]
    if project:
        mask_ref, gnext_ref, bnext_ref, wp_ref = [take() for _ in range(4)]
    if finish:
        z_out = take()
    if project:
        a_in, b_in = take(), take()
    natural_out = not project
    z_ref = take() if natural_in else z_in
    if finish:
        y_buf = take()
        zo_ref = take() if natural_out else z_out
    if project:
        sa, sb, out_a, out_b, send_sem, recv_sem = [take() for _ in range(6)]
    s = pl.program_id(0)
    if project:
        @pl.when(s == 0)
        def _():
            greet(ND)

        row, col = lax.axis_index('dap'), lax.axis_index('dap2')
        rows = pl.ds(pl.multiple_of(s * SL, SL), SL)

        def push(grp):
            for k, (src, dst) in enumerate(((out_a, a_in), (out_b, b_in))):
                team = 8 if project == 'in' and k == 1 else ND
                split = 8 if project == 'in' else ND
                each = 128 // split
                lane = col if team == ND else lax.rem(col, 2)
                lanes = pl.ds(pl.multiple_of(lane * 128, 128), 128)
                there = dst.at[:, row, grp, rows, lanes]

                def part(index):
                    return src.at[s, pl.ds(index * each, each), grp]

                def send(n, carry):
                    other, device = partner(team, n)
                    if team != split:
                        other = device['dap'] * 2 + lax.rem(device['dap2'], 2)
                    pltpu.make_async_remote_copy(
                        src_ref=part(other), dst_ref=there, send_sem=send_sem.at[k], recv_sem=recv_sem.at[k],
                        device_id=device, device_id_type=MESH).start()
                    return carry

                lax.fori_loop(1, team, send, 0)
                pltpu.make_async_copy(part(place(split)), there, recv_sem.at[k]).start()

    if natural_in:
        def load(r, carry):
            for g in range(GR):
                z_ref[g, r] = z_in[g, r, :128]
                z_ref[GR, r, g * 32:(g + 1) * 32] = z_in[g, r, 128:]
            return carry

        lax.fori_loop(0, SL, load, 0)

    def group(grp, carry):
        if finish:
            total = jnp.zeros((SL, 128), F32)
            for cb in range(8):
                total += jnp.sum(t_ref[cb * 16:(cb + 1) * 16, grp].astype(F32), axis=0)
            mean = (total * (1.0 / 128))[None]
            total = jnp.zeros((SL, 128), F32)
            for cb in range(8):
                centered = t_ref[cb * 16:(cb + 1) * 16, grp].astype(F32) - mean
                total += jnp.sum(centered * centered, axis=0)
            scale = lax.rsqrt(total * (1.0 / 128) + NORM_EPS)[None]
            for cb in range(8):
                sl = slice(cb * 16, (cb + 1) * 16)
                y = (t_ref[sl, grp].astype(F32) - mean) * scale * gout_ref[sl] + bout_ref[sl]
                y_buf[cb * 128:(cb + 1) * 128, :] = y.reshape(128, 128)

        def tile(r, inner):
            zf = z_ref[grp, r].astype(F32)
            if finish:
                x = norm_lanes(zf, gin_ref[...], bin_ref[...]).astype(BF16)
                gate = sigmoid(jnp.dot(x, wg_ref[...], preferred_element_type=F32))
                y = y_buf[pl.ds(r, 128, stride=SL), :].astype(BF16)
                update = lax.dot_general(y, wo_ref[...], (((0,), (0,)), ((), ())), preferred_element_type=F32)
                znew = (zf + gate * update).astype(BF16)
                zo_ref[grp, r] = znew
                zf = znew.astype(F32)
            if project:
                x = norm_lanes(zf, gnext_ref[...], bnext_ref[...]).astype(BF16)
                q = lax.dot_general(wp_ref[...], x, (((1,), (1,)), ((), ())), preferred_element_type=F32)
                m = mask_ref[grp, pl.ds(r, 1), :]
                base = pl.multiple_of(r * SWAP, 8)
                sa[pl.ds(base, 128), :] = m * sigmoid(q[128:256]) * q[:128]
                sb[pl.ds(base, 128), :] = m * sigmoid(q[384:]) * q[256:384]
            return inner

        lax.fori_loop(0, SL, tile, 0, unroll=UNROLL)

        if project:
            def swap(cb, inner):
                for u in range(8):
                    c = cb * 8 + u
                    out_a[s, c, grp] = sa[pl.ds(c, SL, stride=SWAP), :].astype(BF16)
                    out_b[s, c, grp] = sb[pl.ds(c, SL, stride=SWAP), :].astype(BF16)
                return inner

            lax.fori_loop(0, 16, swap, 0)

            @pl.when(s == 0)
            def _():
                @pl.when(grp == 0)
                def _():
                    pl.semaphore_wait(pltpu.get_barrier_semaphore(), ND - 1)

                push(grp)
        return carry

    lax.fori_loop(0, 5, group, 0)

    if finish and natural_out:
        def store(r, carry):
            for g in range(GR):
                z_out[g, r, :128] = zo_ref[g, r]
                z_out[g, r, 128:] = zo_ref[GR, r, g * 32:(g + 1) * 32]
            return carry

        lax.fori_loop(0, SL, store, 0)

    if project:
        @pl.when(s > 0)
        def _():
            push(slice(None))

        @pl.when(s == STEPS - 1)
        def _():
            for k, (src, dst) in enumerate(((out_a, a_in), (out_b, b_in))):
                pltpu.make_async_copy(dst, dst, recv_sem.at[k]).wait()
                if project == 'out':
                    sent = src.at[:, pl.ds(0, 128 - 8)]
                elif k == 0:
                    sent = dst.at[pl.ds(0, 15)]
                else:
                    sent = src.at[:, pl.ds(0, 128 - 16)]
                pltpu.make_async_copy(sent, sent, send_sem.at[k]).wait()


def position_call(z, finish_args, project_args, project, collective_id):
    finish, natural_in = finish_args is not None, z.ndim == 4 and z.shape[0] == GR
    full = lambda arr: pl.BlockSpec(arr.shape, lambda s: (0,) * arr.ndim)
    z_spec = pl.BlockSpec((5, SL, 128, 128), lambda s: (0, s, 0, 0))
    n_spec = pl.BlockSpec((GR, SL, B, 128), lambda s: (0, s, 0, 0))
    args, specs = [z], [n_spec if natural_in else z_spec]
    outs, out_specs, scratch = [], [], []
    if natural_in:
        scratch.append(pltpu.VMEM((5, SL, 128, 128), BF16))
    if finish:
        args += list(finish_args)
        specs += [pl.BlockSpec((128, 5, SL, 128), lambda s: (0, 0, s, 0))] + [full(v) for v in finish_args[1:]]
        outs.append(jax.ShapeDtypeStruct((5, RR, 128, 128) if project else (GR, RR, B, 128), BF16))
        out_specs.append(z_spec if project else n_spec)
        scratch.append(pltpu.VMEM((128 * SL, 128), F32))
        if not project:
            scratch.append(pltpu.VMEM((5, SL, 128, 128), BF16))
    if project:
        args += list(project_args)
        specs += [pl.BlockSpec((5, SL, 128), lambda s: (0, s, 0))] + [full(v) for v in project_args[1:]]
        chans = 8 if project == 'out' else 16
        outs += [jax.ShapeDtypeStruct((chans, 4, 5, RR, w), BF16) for w in (512, 512 if project == 'out' else 256)]
        out_specs += [pl.BlockSpec(memory_space=pl.ANY)] * 2
        scratch += [pltpu.VMEM((SWAP * SL, 128), F32)] * 2
        scratch += [pltpu.VMEM((STEPS, 128, 5, SL, 128), BF16)] * 2
        scratch += [pltpu.SemaphoreType.DMA((2,)), pltpu.SemaphoreType.DMA((2,))]
    params = dict(dimension_semantics=('arbitrary',), vmem_limit_bytes=60 * 2 ** 20)
    if project:
        params.update(collective_id=collective_id, has_side_effects=True)
    name = 'position' + ('_finish' if finish else '') + ('_project_' + project if project else '')
    return pl.pallas_call(
        functools.partial(position_kernel, finish, project, natural_in), name=name, grid=(STEPS,),
        in_specs=specs, out_specs=out_specs, out_shape=outs, scratch_shapes=scratch,
        compiler_params=pltpu.CompilerParams(**params))(*args)


def channel_kernel(incoming, a_ref, b_ref, perm_ref, t_in, amat, bmat, tmat, t_out, send_sem, recv_sem):
    c = pl.program_id(0)
    team = 8 if incoming else ND
    each, cols = 128 // team, team // 4
    me = place(team)

    @pl.when(c == 0)
    def _():
        greet(team)

    def rem_columns(ref):
        width = ref.shape[-1]
        packed = ref[0, :, B:, :].astype(F32).reshape(4 * RR, width).astype(BF16)
        return jnp.dot(packed, perm_ref[:width], preferred_element_type=F32)

    def natural(wide, blk):
        return jnp.concatenate([wide[blk * RR:(blk + 1) * RR, g * 128:(g + 1) * 128] for g in range(GR)], axis=0)

    wide = rem_columns(a_ref)
    for blk in range(4):
        amat[blk * B:(blk + 1) * B, :512] = a_ref[0, blk, :B, :]
        amat[blk * B:(blk + 1) * B, 512:] = natural(wide, blk).astype(BF16)
    wide = rem_columns(b_ref)
    for blk in range(4):
        if incoming:
            bmat[blk * B:(blk + 1) * B, :256] = b_ref[0, blk, :B, :]
            bmat[blk * B:(blk + 1) * B, 256:] = natural(wide, blk).astype(BF16)
        else:
            last = natural(wide, blk).astype(BF16)
            bmat[blk * 128:(blk + 1) * 128, :512] = b_ref[0, blk, :128, :]
            bmat[512 + blk * 32:512 + (blk + 1) * 32, :512] = b_ref[0, blk, 128:B, :]
            bmat[blk * 128:(blk + 1) * 128, 512:] = last[:128]
            bmat[512 + blk * 32:512 + (blk + 1) * 32, 512:] = last[128:]
    contract = 0 if incoming else 1
    tmat[...] = lax.dot_general(amat[...], bmat[...], (((contract,), (contract,)), ((), ())), preferred_element_type=F32)

    def rows_of(blk, lanes):
        if incoming:
            return jnp.concatenate([tmat[blk * 128:(blk + 1) * 128, lanes], tmat[512 + blk * 32:512 + (blk + 1) * 32, lanes]], axis=0)
        return tmat[blk * B:(blk + 1) * B, lanes]

    packed = []
    for blk in range(4):
        for j in range(cols):
            t_out[c, blk * cols + j, :B, :] = rows_of(blk, slice(j * 128, (j + 1) * 128)).astype(BF16)
        rem = rows_of(blk, slice(cols * 128, cols * 128 + 128))
        packed.append(jnp.concatenate([rem[g * RR:(g + 1) * RR] for g in range(GR)], axis=1))
    wide = jnp.dot(jnp.concatenate(packed, axis=0).astype(BF16), perm_ref[:, :cols * 128], preferred_element_type=F32)
    for blk in range(4):
        for j in range(cols):
            t_out[c, blk * cols + j, B:, :] = wide[blk * RR:(blk + 1) * RR, j * 128:(j + 1) * 128].astype(BF16)

    @pl.when(c == 0)
    def _():
        pl.semaphore_wait(pltpu.get_barrier_semaphore(), team - 1)

    def send(n, carry):
        other, device = partner(team, n)
        pltpu.make_async_remote_copy(
            src_ref=t_out.at[c, other], dst_ref=t_in.at[me * each + c],
            send_sem=send_sem, recv_sem=recv_sem, device_id=device, device_id_type=MESH).start()
        return carry

    lax.fori_loop(1, team, send, 0)
    pltpu.make_async_copy(t_out.at[c, me], t_in.at[me * each + c], recv_sem).start()

    @pl.when(c == each - 1)
    def _():
        pltpu.make_async_copy(t_in, t_in, recv_sem).wait()
        sent = t_out.at[:, pl.ds(0, team - 1)]
        pltpu.make_async_copy(sent, sent, send_sem).wait()


def channel_call(a_in, b_in, perm, incoming):
    team = 8 if incoming else ND
    each, width = 128 // team, 128 * team // 4
    merge = lambda v: v.reshape(each, 4, 200, v.shape[-1])
    spec = lambda v: pl.BlockSpec((1, 4, 200, v.shape[-1]), lambda c: (c, 0, 0, 0))
    return pl.pallas_call(
        functools.partial(channel_kernel, incoming), name='channel_in' if incoming else 'channel_out', grid=(each,),
        in_specs=[spec(a_in), spec(b_in), pl.BlockSpec((512, 512), lambda c: (0, 0))],
        out_specs=pl.BlockSpec(memory_space=pl.ANY),
        out_shape=jax.ShapeDtypeStruct((128, 200, 128), BF16),
        scratch_shapes=[
            pltpu.VMEM((640, 640), BF16), pltpu.VMEM((640, width + 128), BF16), pltpu.VMEM((640, width + 128), F32),
            pltpu.VMEM((each, team, 200, 128), BF16),
            pltpu.SemaphoreType.DMA, pltpu.SemaphoreType.DMA],
        compiler_params=pltpu.CompilerParams(
            dimension_semantics=('arbitrary',), vmem_limit_bytes=60 * 2 ** 20,
            collective_id=4 if incoming else 3, has_side_effects=True),
    )(merge(a_in), merge(b_in), perm)


def solution(mesh):
    pair_spec = P(('data', 'dap'), 'dap2', None)
    mask_spec = P(('data', 'dap'), 'dap2')

    def local_fn(pair_act, pair_mask, in_gamma, in_beta, w_proj, w_gate, out_gamma, out_beta, w_out):
        mask = to_tiles(pair_mask.astype(F32))
        z = pair_act.reshape(GR, RR, B, 128)
        src = jnp.arange(512)
        perm = (((src % 128) // 32 * 128 + src // 128 * 32 + src % 32)[:, None] == jnp.arange(512)[None, :]).astype(BF16)
        updates = [(layer, u) for layer in range(in_gamma.shape[0]) for u in range(2)]

        def project_args(at):
            return (mask, in_gamma[at][None], in_beta[at][None], w_proj[at].T)

        def finish_args(at, t):
            wide = lambda v: jnp.broadcast_to(v[at][:, None, None], (128, 1, 128))
            return (t.reshape(128, 5, RR, 128), in_gamma[at][None], in_beta[at][None], w_gate[at], wide(out_gamma), wide(out_beta), w_out[at])

        kind = lambda at: 'in' if at[1] else 'out'
        a_in, b_in = position_call(z, None, project_args(updates[0]), 'out', 1)
        for n, at in enumerate(updates):
            t = channel_call(a_in, b_in, perm, at[1] == 1)
            if n + 1 < len(updates):
                after = updates[n + 1]
                ident = 2 if n == 0 else 5 if at[1] else 6
                z, a_in, b_in = position_call(z, finish_args(at, t), project_args(after), kind(after), ident)
            else:
                z, = position_call(z, finish_args(at, t), None, None, None)
        return z.reshape(B, B, 128)

    return jax.shard_map(local_fn, mesh=mesh, in_specs=(pair_spec, mask_spec) + (P(),) * 7, out_specs=pair_spec, check_vma=False)
```

```python
import functools

import jax
import jax.numpy as jnp
from jax import lax
from jax.experimental import pallas as pl
from jax.experimental.pallas import tpu as pltpu
from jax.sharding import PartitionSpec as P

NORM_EPS = 1e-5
F32 = jnp.float32
BF16 = jnp.bfloat16
MESH = pl.DeviceIdType.MESH
ND = 16
B = 160
GR = 4
RR = 40
SL = 8
STEPS = RR // SL
UNROLL = 4
SWAP = 136


def to_tiles(block):
    rest = block.shape[2:]
    grouped = block.reshape((GR, RR, B) + rest)
    main = grouped[:, :, :128]
    rem = jnp.swapaxes(grouped[:, :, 128:], 0, 1).reshape((1, RR, 128) + rest)
    return jnp.concatenate([main, rem], axis=0)


def sigmoid(v):
    return 0.5 * jnp.tanh(0.5 * v) + 0.5


def norm_lanes(values, gamma, beta):
    centered = values - jnp.mean(values, axis=-1, keepdims=True)
    variance = jnp.mean(centered * centered, axis=-1, keepdims=True)
    return centered * lax.rsqrt(variance + NORM_EPS) * gamma + beta


def place(team):
    row, col = lax.axis_index('dap'), lax.axis_index('dap2')
    return row * 4 + col if team == ND else row * 2 + lax.rem(col, 2)


def partner(team, n):
    other = lax.rem(place(team) + n, team)
    if team == ND:
        return other, {'dap': other // 4, 'dap2': lax.rem(other, 4)}
    half = lax.axis_index('dap2') // 2
    return other, {'dap': other // 2, 'dap2': half * 2 + lax.rem(other, 2)}


def greet(team):
    barrier = pltpu.get_barrier_semaphore()

    def signal(n, carry):
        _, device = partner(team, n)
        pl.semaphore_signal(barrier, inc=1, device_id=device, device_id_type=MESH)
        return carry

    lax.fori_loop(1, team, signal, 0)


class Refs:
    pass


def position_step(finish, project, natural_in, s, r):
    natural_out = not project
    z_ref = r.z_own if natural_in else r.z_in
    if finish:
        zo_ref = r.zo_own if natural_out else r.z_out
    if project:
        row, col = lax.axis_index('dap'), lax.axis_index('dap2')
        rows = pl.ds(pl.multiple_of(s * SL, SL), SL)
        pairs = ((r.out_a, r.a_in), (r.out_b, r.b_in))

        def push(grp):
            for k, (src, dst) in enumerate(pairs):
                team = 8 if project == 'in' and k == 1 else ND
                split = 8 if project == 'in' else ND
                each = 128 // split
                lane = col if team == ND else lax.rem(col, 2)
                lanes = pl.ds(pl.multiple_of(lane * 128, 128), 128)
                there = dst.at[:, row, grp, rows, lanes]

                def part(index):
                    return src.at[s, pl.ds(index * each, each), grp]

                def send(n, carry):
                    other, device = partner(team, n)
                    if team != split:
                        other = device['dap'] * 2 + lax.rem(device['dap2'], 2)
                    pltpu.make_async_remote_copy(
                        src_ref=part(other), dst_ref=there, send_sem=r.send_sem.at[k], recv_sem=r.recv_sem.at[k],
                        device_id=device, device_id_type=MESH).start()
                    return carry

                lax.fori_loop(1, team, send, 0)
                pltpu.make_async_copy(part(place(split)), there, r.recv_sem.at[k]).start()

    if natural_in:
        def load(n, carry):
            for g in range(GR):
                z_ref[g, n] = r.z_in[g, n, :128]
                z_ref[GR, n, g * 32:(g + 1) * 32] = r.z_in[g, n, 128:]
            return carry

        lax.fori_loop(0, SL, load, 0)

    def group(grp, carry):
        if finish:
            total = jnp.zeros((SL, 128), F32)
            for cb in range(8):
                total += jnp.sum(r.tri(cb * 16, grp).astype(F32), axis=0)
            mean = (total * (1.0 / 128))[None]
            total = jnp.zeros((SL, 128), F32)
            for cb in range(8):
                centered = r.tri(cb * 16, grp).astype(F32) - mean
                total += jnp.sum(centered * centered, axis=0)
            scale = lax.rsqrt(total * (1.0 / 128) + NORM_EPS)[None]
            for cb in range(8):
                sl = slice(cb * 16, (cb + 1) * 16)
                y = (r.tri(cb * 16, grp).astype(F32) - mean) * scale * r.gout[0, 0, sl] + r.bout[0, 0, sl]
                r.y_buf[cb * 128:(cb + 1) * 128, :] = y.reshape(128, 128)

        def tile(n, inner):
            zf = z_ref[grp, n].astype(F32)
            if finish:
                x = norm_lanes(zf, r.gin[0, 0], r.bin[0, 0]).astype(BF16)
                gate = sigmoid(jnp.dot(x, r.wg[0, 0], preferred_element_type=F32))
                y = r.y_buf[pl.ds(n, 128, stride=SL), :].astype(BF16)
                update = lax.dot_general(y, r.wo[0, 0], (((0,), (0,)), ((), ())), preferred_element_type=F32)
                znew = (zf + gate * update).astype(BF16)
                zo_ref[grp, n] = znew
                zf = znew.astype(F32)
            if project:
                x = norm_lanes(zf, r.gnext[0, 0], r.bnext[0, 0]).astype(BF16)
                q = lax.dot_general(r.wp[0, 0], x, (((1,), (1,)), ((), ())), preferred_element_type=F32)
                m = r.mask[grp, pl.ds(n, 1), :]
                base = pl.multiple_of(n * SWAP, 8)
                r.sa[pl.ds(base, 128), :] = m * sigmoid(q[128:256]) * q[:128]
                r.sb[pl.ds(base, 128), :] = m * sigmoid(q[384:]) * q[256:384]
            return inner

        lax.fori_loop(0, SL, tile, 0, unroll=UNROLL)

        if project:
            def swap(cb, inner):
                for u in range(8):
                    c = cb * 8 + u
                    r.out_a[s, c, grp] = r.sa[pl.ds(c, SL, stride=SWAP), :].astype(BF16)
                    r.out_b[s, c, grp] = r.sb[pl.ds(c, SL, stride=SWAP), :].astype(BF16)
                return inner

            lax.fori_loop(0, 16, swap, 0)

            @pl.when(s == 0)
            def _():
                if not r.greeted:
                    @pl.when(grp == 0)
                    def _():
                        pl.semaphore_wait(pltpu.get_barrier_semaphore(), ND - 1)

                push(grp)
        return carry

    lax.fori_loop(0, 5, group, 0)

    if finish and natural_out:
        def store(n, carry):
            for g in range(GR):
                r.z_out[g, n, :128] = zo_ref[g, n]
                r.z_out[g, n, 128:] = zo_ref[GR, n, g * 32:(g + 1) * 32]
            return carry

        lax.fori_loop(0, SL, store, 0)

    if project:
        @pl.when(s > 0)
        def _():
            push(slice(None))

        @pl.when(s == STEPS - 1)
        def _():
            for k, (src, dst) in enumerate(pairs):
                pltpu.make_async_copy(dst, dst, r.recv_sem.at[k]).wait()
                if project == 'out':
                    sent = src.at[:, pl.ds(0, 128 - 8)]
                elif k == 0:
                    sent = dst.at[pl.ds(0, 15)]
                else:
                    sent = src.at[:, pl.ds(0, 128 - 16)]
                pltpu.make_async_copy(sent, sent, r.send_sem.at[k]).wait()


def channel_step(incoming, r, put_main, put_rem):
    cols = 2 if incoming else 4

    def rem_columns(ref):
        width = ref.shape[-1]
        packed = ref[0, :, B:, :].astype(F32).reshape(4 * RR, width).astype(BF16)
        return jnp.dot(packed, r.perm[:width], preferred_element_type=F32)

    def natural(wide, blk):
        return jnp.concatenate([wide[blk * RR:(blk + 1) * RR, g * 128:(g + 1) * 128] for g in range(GR)], axis=0)

    wide = rem_columns(r.a)
    for blk in range(4):
        r.amat[blk * B:(blk + 1) * B, :512] = r.a[0, blk, :B, :]
        r.amat[blk * B:(blk + 1) * B, 512:] = natural(wide, blk).astype(BF16)
    wide = rem_columns(r.b)
    for blk in range(4):
        last = natural(wide, blk).astype(BF16)
        if incoming:
            r.bmat[blk * B:(blk + 1) * B, :256] = r.b[0, blk, :B, :]
            r.bmat[blk * B:(blk + 1) * B, 256:] = last
        else:
            r.bmat[blk * 128:(blk + 1) * 128, :512] = r.b[0, blk, :128, :]
            r.bmat[512 + blk * 32:512 + (blk + 1) * 32, :512] = r.b[0, blk, 128:B, :]
            r.bmat[blk * 128:(blk + 1) * 128, 512:] = last[:128]
            r.bmat[512 + blk * 32:512 + (blk + 1) * 32, 512:] = last[128:]
    contract = 0 if incoming else 1
    r.tmat[...] = lax.dot_general(r.amat[...], r.bmat[...], (((contract,), (contract,)), ((), ())), preferred_element_type=F32)

    def rows_of(blk, lanes):
        if incoming:
            return jnp.concatenate([r.tmat[blk * 128:(blk + 1) * 128, lanes], r.tmat[512 + blk * 32:512 + (blk + 1) * 32, lanes]], axis=0)
        return r.tmat[blk * B:(blk + 1) * B, lanes]

    packed = []
    for blk in range(4):
        for j in range(cols):
            put_main(blk * cols + j, rows_of(blk, slice(j * 128, (j + 1) * 128)))
        rem = rows_of(blk, slice(cols * 128, cols * 128 + 128))
        packed.append(jnp.concatenate([rem[g * RR:(g + 1) * RR] for g in range(GR)], axis=1))
    wide = jnp.dot(jnp.concatenate(packed, axis=0).astype(BF16), r.perm[:, :cols * 128], preferred_element_type=F32)
    for blk in range(4):
        for j in range(cols):
            put_rem(blk * cols + j, wide[blk * RR:(blk + 1) * RR, j * 128:(j + 1) * 128])


def channel_out_kernel(a_ref, b_ref, perm_ref, t_in, amat, bmat, tmat, t_out, send_sem, recv_sem):
    r = Refs()
    r.a, r.b, r.perm, r.amat, r.bmat, r.tmat = a_ref, b_ref, perm_ref, amat, bmat, tmat
    c = pl.program_id(0)
    me = place(ND)

    @pl.when(c == 0)
    def _():
        greet(ND)

    def put_main(owner, v):
        t_out[c, owner, :B, :] = v.astype(BF16)

    def put_rem(owner, v):
        t_out[c, owner, B:, :] = v.astype(BF16)

    channel_step(False, r, put_main, put_rem)

    @pl.when(c == 0)
    def _():
        pl.semaphore_wait(pltpu.get_barrier_semaphore(), ND - 1)

    def send(n, carry):
        other, device = partner(ND, n)
        pltpu.make_async_remote_copy(
            src_ref=t_out.at[c, other], dst_ref=t_in.at[me * 8 + c],
            send_sem=send_sem, recv_sem=recv_sem, device_id=device, device_id_type=MESH).start()
        return carry

    lax.fori_loop(1, ND, send, 0)
    pltpu.make_async_copy(t_out.at[c, me], t_in.at[me * 8 + c], recv_sem).start()

    @pl.when(c == 7)
    def _():
        pltpu.make_async_copy(t_in, t_in, recv_sem).wait()
        sent = t_out.at[:, pl.ds(0, ND - 1)]
        pltpu.make_async_copy(sent, sent, send_sem).wait()


def fused_kernel(channels, finish, project, natural_in, *refs):
    refs = list(refs)
    take = lambda: refs.pop(0)
    r = Refs()
    if channels:
        r.a, r.b, r.perm = take(), take(), take()
    r.z_in = take()
    if finish:
        if not channels:
            t_ref = take()
            r.tri = lambda c0, grp: t_ref[c0:c0 + 16, grp]
        r.gin, r.bin, r.wg, r.gout, r.bout, r.wo = [take() for _ in range(6)]
    if project:
        r.mask, r.gnext, r.bnext, r.wp = [take() for _ in range(4)]
    if finish:
        r.z_out = take()
    if project:
        r.a_in, r.b_in = take(), take()
    if natural_in:
        r.z_own = take()
    if finish:
        r.y_buf = take()
        if not project:
            r.zo_own = take()
    if project:
        r.sa, r.sb, r.out_a, r.out_b, r.send_sem, r.recv_sem = [take() for _ in range(6)]
    step = pl.program_id(0)
    team = ND if project else 8
    if project or channels:
        @pl.when(step == 0)
        def _():
            greet(team)
    r.greeted = channels
    if not channels:
        position_step(finish, project, natural_in, step, r)
        return
    r.amat, r.bmat, r.tmat, t_out, t_own, send_t, recv_t = [take() for _ in range(7)]
    me = place(8)

    @pl.when(step < 16)
    def _():
        def put_main(owner, v):
            tiles = v.reshape(GR, STEPS, SL, 128).astype(BF16)
            for s in range(STEPS):
                t_out[step, owner, s, :GR] = tiles[:, s]

        def put_rem(owner, v):
            t_out[step, owner, :, GR] = v.reshape(STEPS, SL, 128).astype(BF16)

        channel_step(True, r, put_main, put_rem)
        t_own[me * 16 + step] = t_out[step, me]

    @pl.when(step == 15)
    def _():
        pl.semaphore_wait(pltpu.get_barrier_semaphore(), team - 1)

        def slab(s, carry):
            def send(n, inner):
                other, device = partner(8, n)
                pltpu.make_async_remote_copy(
                    src_ref=t_out.at[:, other, s], dst_ref=t_own.at[pl.ds(me * 16, 16), s],
                    send_sem=send_t, recv_sem=recv_t.at[s], device_id=device, device_id_type=MESH).start()
                return inner

            return lax.fori_loop(1, 8, send, carry)

        lax.fori_loop(0, STEPS, slab, 0)

    @pl.when(step >= 16)
    def _():
        s = step - 16
        landed = t_own.at[pl.ds(0, 112), s]
        pltpu.make_async_copy(landed, landed, recv_t.at[s]).wait()
        r.tri = lambda c0, grp: t_own[c0:c0 + 16, s, grp]
        position_step(finish, project, natural_in, s, r)

    @pl.when(step == 16 + STEPS - 1)
    def _():
        sent = t_out.at[:, pl.ds(0, 7)]
        pltpu.make_async_copy(sent, sent, send_t).wait()


def fused_call(z, at, t, params, after, channels, collective_id):
    finish, project = at is not None, None if after is None else 'in' if after[1] else 'out'
    natural_in = z.shape[0] == GR
    first = 16 if channels else 0
    slab = lambda n: jnp.maximum(n - first, 0) if channels else n
    z_spec = pl.BlockSpec((5, SL, 128, 128), lambda n: (0, slab(n), 0, 0))
    n_spec = pl.BlockSpec((GR, SL, B, 128), lambda n: (0, slab(n), 0, 0))

    def weight(name, which):
        arr = params[name]
        return arr, pl.BlockSpec((1, 1) + arr.shape[2:], lambda n: tuple(which) + (0,) * (arr.ndim - 2))

    ins, outs, scratch = [], [], []
    if channels:
        a_in, b_in, perm = t
        for v in (a_in, b_in):
            v = v.reshape(16, 4, 200, v.shape[-1])
            ins.append((v, pl.BlockSpec((1,) + v.shape[1:], lambda n: (jnp.minimum(n, 15), 0, 0, 0))))
        ins.append((perm, pl.BlockSpec((512, 512), lambda n: (0, 0))))
    ins.append((z, n_spec if natural_in else z_spec))
    if natural_in:
        scratch.append(pltpu.VMEM((5, SL, 128, 128), BF16))
    if finish:
        if not channels:
            ins.append((t.reshape(128, 5, RR, 128), pl.BlockSpec((128, 5, SL, 128), lambda n: (0, 0, n, 0))))
        ins += [weight(name, at) for name in ('gin', 'bin', 'wg', 'gout', 'bout', 'wo')]
        outs.append((jax.ShapeDtypeStruct((5, RR, 128, 128) if project else (GR, RR, B, 128), BF16), z_spec if project else n_spec))
        scratch.append(pltpu.VMEM((128 * SL, 128), F32))
        if not project:
            scratch.append(pltpu.VMEM((5, SL, 128, 128), BF16))
    if project:
        ins.append((params['mask'], pl.BlockSpec((5, SL, 128), lambda n: (0, slab(n), 0))))
        ins += [weight(name, after) for name in ('gin', 'bin', 'wp')]
        chans = 8 if project == 'out' else 16
        anywhere = pl.BlockSpec(memory_space=pl.ANY)
        outs += [(jax.ShapeDtypeStruct((chans, 4, 5, RR, w), BF16), anywhere) for w in (512, 512 if project == 'out' else 256)]
        scratch += [pltpu.VMEM((SWAP * SL, 128), F32)] * 2
        scratch += [pltpu.VMEM((STEPS, 128, 5, SL, 128), BF16)] * 2
        scratch += [pltpu.SemaphoreType.DMA((2,)), pltpu.SemaphoreType.DMA((2,))]
    if channels:
        scratch += [pltpu.VMEM((640, 640), BF16), pltpu.VMEM((640, 384), BF16), pltpu.VMEM((640, 384), F32)]
        scratch += [pltpu.VMEM((16, 8, STEPS, 5, SL, 128), BF16), pltpu.VMEM((128, STEPS, 5, SL, 128), BF16)]
        scratch += [pltpu.SemaphoreType.DMA, pltpu.SemaphoreType.DMA((STEPS,))]
    extra = dict(dimension_semantics=('arbitrary',), vmem_limit_bytes=60 * 2 ** 20)
    if project or channels:
        extra.update(collective_id=collective_id, has_side_effects=True)
    name = '_'.join((['channels'] if channels else []) + (['finish'] if finish else []) + (['project', project] if project else []))
    return pl.pallas_call(
        functools.partial(fused_kernel, channels, finish, project, natural_in), name=name, grid=(first + STEPS,),
        in_specs=[spec for _, spec in ins], out_specs=[spec for _, spec in outs], out_shape=[shape for shape, _ in outs],
        scratch_shapes=scratch, compiler_params=pltpu.CompilerParams(**extra))(*[v for v, _ in ins])


def channel_call(a_in, b_in, perm):
    merge = lambda v: v.reshape(8, 4, 200, 512)
    spec = pl.BlockSpec((1, 4, 200, 512), lambda c: (c, 0, 0, 0))
    return pl.pallas_call(
        channel_out_kernel, name='channels_out', grid=(8,),
        in_specs=[spec, spec, pl.BlockSpec((512, 512), lambda c: (0, 0))],
        out_specs=pl.BlockSpec(memory_space=pl.ANY),
        out_shape=jax.ShapeDtypeStruct((128, 200, 128), BF16),
        scratch_shapes=[
            pltpu.VMEM((640, 640), BF16), pltpu.VMEM((640, 640), BF16), pltpu.VMEM((640, 640), F32),
            pltpu.VMEM((8, ND, 200, 128), BF16),
            pltpu.SemaphoreType.DMA, pltpu.SemaphoreType.DMA],
        compiler_params=pltpu.CompilerParams(
            dimension_semantics=('arbitrary',), vmem_limit_bytes=60 * 2 ** 20, collective_id=3, has_side_effects=True),
    )(merge(a_in), merge(b_in), perm)


def solution(mesh):
    pair_spec = P(('data', 'dap'), 'dap2', None)
    mask_spec = P(('data', 'dap'), 'dap2')

    def local_fn(pair_act, pair_mask, in_gamma, in_beta, w_proj, w_gate, out_gamma, out_beta, w_out):
        mask = to_tiles(pair_mask.astype(F32))
        z = pair_act.reshape(GR, RR, B, 128)
        src = jnp.arange(512)
        perm = (((src % 128) // 32 * 128 + src // 128 * 32 + src % 32)[:, None] == jnp.arange(512)[None, :]).astype(BF16)
        rowed = lambda v: v[:, :, None, :]
        wide = lambda v: jnp.broadcast_to(v[..., None, None], v.shape + (1, 128))
        params = dict(
            mask=mask, gin=rowed(in_gamma), bin=rowed(in_beta), wp=jnp.swapaxes(w_proj, 2, 3), wg=w_gate,
            gout=wide(out_gamma), bout=wide(out_beta), wo=w_out)
        layers = in_gamma.shape[0]
        a_in, b_in = fused_call(z, None, None, params, (0, 0), False, 1)
        for layer in range(layers):
            t = channel_call(a_in, b_in, perm)
            z, a_in, b_in = fused_call(z, (layer, 0), t, params, (layer, 1), False, 2 if layer == 0 else 4)
            if layer + 1 < layers:
                z, a_in, b_in = fused_call(z, (layer, 1), (a_in, b_in, perm), params, (layer + 1, 0), True, 5)
            else:
                z, = fused_call(z, (layer, 1), (a_in, b_in, perm), params, None, True, 6)
        return z.reshape(B, B, 128)

    return jax.shard_map(local_fn, mesh=mesh, in_specs=(pair_spec, mask_spec) + (P(),) * 7, out_specs=pair_spec, check_vma=False)
```

```python
import functools

import jax
import jax.numpy as jnp
from jax import lax
from jax.experimental import pallas as pl
from jax.experimental.pallas import tpu as pltpu
from jax.sharding import PartitionSpec as P

NORM_EPS = 1e-5
F32 = jnp.float32
BF16 = jnp.bfloat16
MESH = pl.DeviceIdType.MESH
ND = 16
B = 160
GR = 4
RR = 40
SL = 8
STEPS = RR // SL
UNROLL = 4
SPLIT = (2, 4, 8, 8)
SWAP = 136


def to_tiles(block):
    rest = block.shape[2:]
    grouped = block.reshape((GR, RR, B) + rest)
    main = grouped[:, :, :128]
    rem = jnp.swapaxes(grouped[:, :, 128:], 0, 1).reshape((1, RR, 128) + rest)
    return jnp.concatenate([main, rem], axis=0)


def sigmoid(v):
    return 0.5 * jnp.tanh(0.5 * v) + 0.5


def norm_lanes(values, gamma, beta):
    centered = values - jnp.mean(values, axis=-1, keepdims=True)
    variance = jnp.mean(centered * centered, axis=-1, keepdims=True)
    return centered * lax.rsqrt(variance + NORM_EPS) * gamma + beta


def place(team):
    row, col = lax.axis_index('dap'), lax.axis_index('dap2')
    return row * 4 + col if team == ND else row * 2 + lax.rem(col, 2)


def partner(team, n):
    other = lax.rem(place(team) + n, team)
    if team == ND:
        return other, {'dap': other // 4, 'dap2': lax.rem(other, 4)}
    half = lax.axis_index('dap2') // 2
    return other, {'dap': other // 2, 'dap2': half * 2 + lax.rem(other, 2)}


def greet(team):
    barrier = pltpu.get_barrier_semaphore()

    def signal(n, carry):
        _, device = partner(team, n)
        pl.semaphore_signal(barrier, inc=1, device_id=device, device_id_type=MESH)
        return carry

    lax.fori_loop(1, team, signal, 0)


class Refs:
    pass


WHOLE = 3


def channel_groups(kind):
    each = 16 if kind == 'in' else 8
    sizes = [each // n for n in SPLIT]
    return tuple((sum(sizes[:n]), sizes[n]) for n in range(len(SPLIT)))


def group_bytes(ref, q):
    if q == 0:
        return ref.at[:, :, pl.ds(0, 4)]
    return ref.at[pl.ds(0, 2 * ref.shape[0] // SPLIT[q]), :, pl.ds(0, 1)]


def position_step(finish, project, natural_in, s, r):
    natural_out = not project
    z_ref = r.z_own if natural_in else r.z_in
    if finish:
        zo_ref = r.zo_own if natural_out else r.z_out
    if project:
        row, col = lax.axis_index('dap'), lax.axis_index('dap2')
        pairs = ((r.out_a, r.a_in), (r.out_b, r.b_in))

        def push(q, slab, grp):
            start, count = (0, 16 if project == 'in' else 8) if q is None else channel_groups(project)[q]
            sem = 0 if q is None else q
            rows = pl.ds(pl.multiple_of(slab * SL, SL), SL)
            for k, (src, dst) in enumerate(pairs):
                team = 8 if project == 'in' and k == 1 else ND
                split = 8 if project == 'in' else ND
                each = 128 // split
                lane = col if team == ND else lax.rem(col, 2)
                lanes = pl.ds(pl.multiple_of(lane * 128, 128), 128)
                there = dst.at[pl.ds(start, count), row, grp, rows, lanes]

                def part(index):
                    return src.at[slab, pl.ds(index * each + start, count), grp]

                def send(n, carry):
                    other, device = partner(team, n)
                    if team != split:
                        other = device['dap'] * 2 + lax.rem(device['dap2'], 2)
                    pltpu.make_async_remote_copy(
                        src_ref=part(other), dst_ref=there, send_sem=r.send_sem.at[k], recv_sem=r.recv_sem.at[k, sem],
                        device_id=device, device_id_type=MESH).start()
                    return carry

                lax.fori_loop(1, team, send, 0)
                pltpu.make_async_copy(part(place(split)), there, r.recv_sem.at[k, sem]).start()

    if natural_in:
        def load(n, carry):
            for g in range(GR):
                z_ref[g, n] = r.z_in[g, n, :128]
                z_ref[GR, n, g * 32:(g + 1) * 32] = r.z_in[g, n, 128:]
            return carry

        lax.fori_loop(0, SL, load, 0)

    def group(grp, carry):
        if finish:
            @pl.when(s == 0)
            def _():
                r.arrive(grp)

            total = jnp.zeros((SL, 128), F32)
            for cb in range(8):
                total += jnp.sum(r.tri(cb * 16, grp).astype(F32), axis=0)
            mean = (total * (1.0 / 128))[None]
            total = jnp.zeros((SL, 128), F32)
            for cb in range(8):
                centered = r.tri(cb * 16, grp).astype(F32) - mean
                total += jnp.sum(centered * centered, axis=0)
            scale = lax.rsqrt(total * (1.0 / 128) + NORM_EPS)[None]
            for cb in range(8):
                sl = slice(cb * 16, (cb + 1) * 16)
                y = (r.tri(cb * 16, grp).astype(F32) - mean) * scale * r.gout[0, 0, sl] + r.bout[0, 0, sl]
                r.y_buf[cb * 128:(cb + 1) * 128, :] = y.reshape(128, 128)

        def tile(n, inner):
            zf = z_ref[grp, n].astype(F32)
            if finish:
                x = norm_lanes(zf, r.gin[0, 0], r.bin[0, 0]).astype(BF16)
                gate = sigmoid(jnp.dot(x, r.wg[0, 0], preferred_element_type=F32))
                y = r.y_buf[pl.ds(n, 128, stride=SL), :].astype(BF16)
                update = lax.dot_general(y, r.wo[0, 0], (((0,), (0,)), ((), ())), preferred_element_type=F32)
                znew = (zf + gate * update).astype(BF16)
                zo_ref[grp, n] = znew
                zf = znew.astype(F32)
            if project:
                x = norm_lanes(zf, r.gnext[0, 0], r.bnext[0, 0]).astype(BF16)
                q = lax.dot_general(r.wp[0, 0], x, (((1,), (1,)), ((), ())), preferred_element_type=F32)
                m = r.mask[grp, pl.ds(n, 1), :]
                base = pl.multiple_of(n * SWAP, 8)
                r.sa[pl.ds(base, 128), :] = m * sigmoid(q[128:256]) * q[:128]
                r.sb[pl.ds(base, 128), :] = m * sigmoid(q[384:]) * q[256:384]
            return inner

        lax.fori_loop(0, SL, tile, 0, unroll=UNROLL)

        if project:
            def swap(cb, inner):
                for u in range(8):
                    c = cb * 8 + u
                    r.out_a[s, c, grp] = r.sa[pl.ds(c, SL, stride=SWAP), :].astype(BF16)
                    r.out_b[s, c, grp] = r.sb[pl.ds(c, SL, stride=SWAP), :].astype(BF16)
                return inner

            lax.fori_loop(0, 16, swap, 0)

            @pl.when(s == 0)
            def _():
                if not finish:
                    @pl.when(grp == 0)
                    def _():
                        pl.semaphore_wait(pltpu.get_barrier_semaphore(), ND - 1)

                push(None, s, grp)
        return carry

    lax.fori_loop(0, 5, group, 0)

    if finish and natural_out:
        def store(n, carry):
            for g in range(GR):
                r.z_out[g, n, :128] = zo_ref[g, n]
                r.z_out[g, n, 128:] = zo_ref[GR, n, g * 32:(g + 1) * 32]
            return carry

        lax.fori_loop(0, SL, store, 0)

    if project:
        @pl.when((s > 0) & (s < WHOLE))
        def _():
            push(None, s, slice(None))

        @pl.when(s >= WHOLE)
        def _():
            push(0, s, slice(None))

        @pl.when(s == STEPS - 1)
        def _():
            for q in range(1, len(channel_groups(project))):
                def later(slab, carry):
                    push(q, slab, slice(None))
                    return carry

                lax.fori_loop(WHOLE, STEPS, later, 0)


def channel_step(incoming, r, put_main, put_rem):
    cols = 2 if incoming else 4

    def rem_columns(ref):
        width = ref.shape[-1]
        packed = ref[0, :, B:, :].astype(F32).reshape(4 * RR, width).astype(BF16)
        return jnp.dot(packed, r.perm[:width], preferred_element_type=F32)

    def natural(wide, blk):
        return jnp.concatenate([wide[blk * RR:(blk + 1) * RR, g * 128:(g + 1) * 128] for g in range(GR)], axis=0)

    wide = rem_columns(r.a)
    for blk in range(4):
        r.amat[blk * B:(blk + 1) * B, :512] = r.a[0, blk, :B, :]
        r.amat[blk * B:(blk + 1) * B, 512:] = natural(wide, blk).astype(BF16)
    wide = rem_columns(r.b)
    for blk in range(4):
        last = natural(wide, blk).astype(BF16)
        if incoming:
            r.bmat[blk * B:(blk + 1) * B, :256] = r.b[0, blk, :B, :]
            r.bmat[blk * B:(blk + 1) * B, 256:] = last
        else:
            r.bmat[blk * 128:(blk + 1) * 128, :512] = r.b[0, blk, :128, :]
            r.bmat[512 + blk * 32:512 + (blk + 1) * 32, :512] = r.b[0, blk, 128:B, :]
            r.bmat[blk * 128:(blk + 1) * 128, 512:] = last[:128]
            r.bmat[512 + blk * 32:512 + (blk + 1) * 32, 512:] = last[128:]
    contract = 0 if incoming else 1
    r.tmat[...] = lax.dot_general(r.amat[...], r.bmat[...], (((contract,), (contract,)), ((), ())), preferred_element_type=F32)

    def rows_of(blk, lanes):
        if incoming:
            return jnp.concatenate([r.tmat[blk * 128:(blk + 1) * 128, lanes], r.tmat[512 + blk * 32:512 + (blk + 1) * 32, lanes]], axis=0)
        return r.tmat[blk * B:(blk + 1) * B, lanes]

    packed = []
    for blk in range(4):
        for j in range(cols):
            put_main(blk * cols + j, rows_of(blk, slice(j * 128, (j + 1) * 128)))
        rem = rows_of(blk, slice(cols * 128, cols * 128 + 128))
        packed.append(jnp.concatenate([rem[g * RR:(g + 1) * RR] for g in range(GR)], axis=1))
    wide = jnp.dot(jnp.concatenate(packed, axis=0).astype(BF16), r.perm[:, :cols * 128], preferred_element_type=F32)
    for blk in range(4):
        for j in range(cols):
            put_rem(blk * cols + j, wide[blk * RR:(blk + 1) * RR, j * 128:(j + 1) * 128])


def update_kernel(finish, project, natural_in, *refs):
    refs = list(refs)
    take = lambda: refs.pop(0)
    r = Refs()
    r.z_in = take()
    if finish:
        t_ref = take()
        r.gin, r.bin, r.wg, r.gout, r.bout, r.wo = [take() for _ in range(6)]
    if project:
        r.perm, r.mask, r.gnext, r.bnext, r.wp = [take() for _ in range(5)]
    if finish:
        r.z_out = take()
    if project:
        t_out, r.a_in, r.b_in = [take() for _ in range(3)]
    if natural_in:
        r.z_own = take()
    if finish:
        r.y_buf, t_own, send_t, recv_t = [take() for _ in range(4)]
        if not project:
            r.zo_own = take()
    if project:
        r.sa, r.sb, r.out_a, r.out_b, r.send_sem, r.recv_sem = [take() for _ in range(6)]
        r.amat, r.bmat, r.tmat, abuf, bbuf, fetch_sem = [take() for _ in range(6)]
    step = pl.program_id(0)

    @pl.when(step == 0)
    def _():
        team = 8 if finish == 'in' else ND
        met = ND if project else team
        greet(met)
        if finish:
            pl.semaphore_wait(pltpu.get_barrier_semaphore(), met - 1)
            each, me = 128 // team, place(team)

            def give(s, grp, sem):
                there = t_own.at[pl.ds(me * each, each), s, grp]

                def send(n, inner):
                    other, device = partner(team, n)
                    pltpu.make_async_remote_copy(
                        src_ref=t_ref.at[:, other, s, grp], dst_ref=there, send_sem=send_t, recv_sem=recv_t.at[sem],
                        device_id=device, device_id_type=MESH).start()
                    return inner

                lax.fori_loop(1, team, send, 0)
                pltpu.make_async_copy(t_ref.at[:, me, s, grp], there, recv_t.at[sem]).start()

            def piece(grp, carry):
                give(0, grp, STEPS + grp)
                return carry

            def slab(s, carry):
                give(s, slice(None), s)
                return carry

            lax.fori_loop(0, 5, piece, 0)
            lax.fori_loop(1, STEPS, slab, 0)

    @pl.when(step < STEPS)
    def _():
        if finish:
            @pl.when(step > 0)
            def _():
                landed = t_own.at[:, step]
                pltpu.make_async_copy(landed, landed, recv_t.at[step]).wait()

            def arrive(grp):
                landed = t_own.at[:, 0, grp]
                pltpu.make_async_copy(landed, landed, recv_t.at[STEPS + grp]).wait()

            r.arrive = arrive
            r.tri = lambda c0, grp: t_own[c0:c0 + 16, step, grp]
        position_step(finish, project, natural_in, step, r)

    if project:
        @pl.when(step >= STEPS)
        def _():
            c = step - STEPS
            each = 16 if project == 'in' else 8
            pairs = ((r.a_in, abuf), (r.b_in, bbuf))

            def fetch(chan):
                slot = lax.rem(chan, 2)
                for k, (src, buf) in enumerate(pairs):
                    for g in range(5):
                        pltpu.make_async_copy(src.at[chan, :, g], buf.at[slot, :, pl.ds(g * RR, RR)], fetch_sem.at[k, slot]).start()

            groups = channel_groups(project)
            for q, (start, count) in enumerate(groups):
                @pl.when(c == start)
                def _():
                    for k, (src, _) in enumerate(pairs):
                        landed = group_bytes(src, q)
                        pltpu.make_async_copy(landed, landed, r.recv_sem.at[k, q]).wait()
                    fetch(c)

            slot = lax.rem(c, 2)
            for k, (_, buf) in enumerate(pairs):
                pltpu.make_async_copy(buf.at[slot], buf.at[slot], fetch_sem.at[k, slot]).wait()
            last = functools.reduce(lambda x, y: x | y, [c == start + count - 1 for start, count in groups])

            @pl.when(jnp.logical_not(last))
            def _():
                fetch(c + 1)

            r.a, r.b = abuf.at[pl.ds(slot, 1)], bbuf.at[pl.ds(slot, 1)]

            def put_main(owner, v):
                tiles = v.reshape(GR, STEPS, SL, 128).astype(BF16)
                for s in range(STEPS):
                    t_out[0, owner, s, :GR] = tiles[:, s]

            def put_rem(owner, v):
                t_out[0, owner, :, GR] = v.reshape(STEPS, SL, 128).astype(BF16)

            channel_step(project == 'in', r, put_main, put_rem)

            @pl.when(c == each - 1)
            def _():
                for k, (src, dst) in enumerate(((r.out_a, r.a_in), (r.out_b, r.b_in))):
                    if project == 'out':
                        sent = src.at[:, pl.ds(0, 128 - 8)]
                    elif k == 0:
                        sent = dst.at[pl.ds(0, 15)]
                    else:
                        sent = src.at[:, pl.ds(0, 128 - 16)]
                    pltpu.make_async_copy(sent, sent, r.send_sem.at[k]).wait()

    if finish:
        @pl.when(step == STEPS - 1)
        def _():
            team = 8 if finish == 'in' else ND
            sent = t_own.at[pl.ds(0, 128 - 128 // team)]
            pltpu.make_async_copy(sent, sent, send_t).wait()


def update_call(z, t, at, after, params, collective_id):
    kind = lambda which: None if which is None else 'in' if which[1] else 'out'
    finish, project = kind(at), kind(after)
    natural_in = z.shape[0] == GR
    slab = lambda n: jnp.minimum(n, STEPS - 1)
    z_spec = pl.BlockSpec((5, SL, 128, 128), lambda n: (0, slab(n), 0, 0))
    n_spec = pl.BlockSpec((GR, SL, B, 128), lambda n: (0, slab(n), 0, 0))
    anywhere = pl.BlockSpec(memory_space=pl.ANY)

    def weight(name, which):
        arr = params[name]
        return arr, pl.BlockSpec((1, 1) + arr.shape[2:], lambda n: tuple(which) + (0,) * (arr.ndim - 2))

    ins, outs, scratch, steps = [(z, n_spec if natural_in else z_spec)], [], [], STEPS
    if natural_in:
        scratch.append(pltpu.VMEM((5, SL, 128, 128), BF16))
    if finish:
        ins.append((t, anywhere))
        ins += [weight(name, at) for name in ('gin', 'bin', 'wg', 'gout', 'bout', 'wo')]
        outs.append((jax.ShapeDtypeStruct((5, RR, 128, 128) if project else (GR, RR, B, 128), BF16), z_spec if project else n_spec))
        scratch += [pltpu.VMEM((128 * SL, 128), F32), pltpu.VMEM((128, STEPS, 5, SL, 128), BF16)]
        scratch += [pltpu.SemaphoreType.DMA, pltpu.SemaphoreType.DMA((STEPS + 5,))]
        if not project:
            scratch.append(pltpu.VMEM((5, SL, 128, 128), BF16))
    if project:
        ins.append((params['perm'], pl.BlockSpec((512, 512), lambda n: (0, 0))))
        ins.append((params['mask'], pl.BlockSpec((5, SL, 128), lambda n: (0, slab(n), 0))))
        ins += [weight(name, after) for name in ('gin', 'bin', 'wp')]
        each, owners, width = (8, 16, 512) if project == 'out' else (16, 8, 256)
        steps += each
        outs.append((jax.ShapeDtypeStruct((each, owners, STEPS, 5, SL, 128), BF16),
                     pl.BlockSpec((1, owners, STEPS, 5, SL, 128), lambda n: (jnp.maximum(n - STEPS, 0), 0, 0, 0, 0, 0))))
        outs += [(jax.ShapeDtypeStruct((each, 4, 5, RR, w), BF16), anywhere) for w in (512, width)]
        scratch += [pltpu.VMEM((SWAP * SL, 128), F32)] * 2
        scratch += [pltpu.VMEM((STEPS, 128, 5, SL, 128), BF16)] * 2
        scratch += [pltpu.SemaphoreType.DMA((2,)), pltpu.SemaphoreType.DMA((2, len(SPLIT)))]
        scratch += [pltpu.VMEM((640, 640), BF16), pltpu.VMEM((640, width + 128), BF16), pltpu.VMEM((640, width + 128), F32)]
        scratch += [pltpu.VMEM((2, 4, 200, w), BF16) for w in (512, width)] + [pltpu.SemaphoreType.DMA((2, 2))]
    name = '_'.join((['finish', finish] if finish else []) + (['start', project] if project else []))
    return pl.pallas_call(
        functools.partial(update_kernel, finish, project, natural_in), name=name, grid=(steps,),
        in_specs=[spec for _, spec in ins], out_specs=[spec for _, spec in outs], out_shape=[shape for shape, _ in outs],
        scratch_shapes=scratch, compiler_params=pltpu.CompilerParams(
            dimension_semantics=('arbitrary',), vmem_limit_bytes=60 * 2 ** 20, collective_id=collective_id, has_side_effects=True),
    )(*[v for v, _ in ins])


def solution(mesh):
    pair_spec = P(('data', 'dap'), 'dap2', None)
    mask_spec = P(('data', 'dap'), 'dap2')

    def local_fn(pair_act, pair_mask, in_gamma, in_beta, w_proj, w_gate, out_gamma, out_beta, w_out):
        mask = to_tiles(pair_mask.astype(F32))
        z = pair_act.reshape(GR, RR, B, 128)
        src = jnp.arange(512)
        perm = (((src % 128) // 32 * 128 + src // 128 * 32 + src % 32)[:, None] == jnp.arange(512)[None, :]).astype(BF16)
        rowed = lambda v: v[:, :, None, :]
        wide = lambda v: jnp.broadcast_to(v[..., None, None], v.shape + (1, 128))
        params = dict(
            perm=perm, mask=mask, gin=rowed(in_gamma), bin=rowed(in_beta), wp=jnp.swapaxes(w_proj, 2, 3), wg=w_gate,
            gout=wide(out_gamma), bout=wide(out_beta), wo=w_out)
        layers = in_gamma.shape[0]
        t, _, _ = update_call(z, None, None, (0, 0), params, 1)
        for layer in range(layers):
            z, t, _, _ = update_call(z, t, (layer, 0), (layer, 1), params, 2 if layer == 0 else 3)
            if layer + 1 < layers:
                z, t, _, _ = update_call(z, t, (layer, 1), (layer + 1, 0), params, 4)
            else:
                z, = update_call(z, t, (layer, 1), None, params, 5)
        return z.reshape(B, B, 128)

    return jax.shard_map(local_fn, mesh=mesh, in_specs=(pair_spec, mask_spec) + (P(),) * 7, out_specs=pair_spec, check_vma=False)
```

```python
import functools

import jax
import jax.numpy as jnp
from jax import lax
from jax.experimental import pallas as pl
from jax.experimental.pallas import tpu as pltpu
from jax.sharding import PartitionSpec as P

NORM_EPS = 1e-5
F32 = jnp.float32
BF16 = jnp.bfloat16
MESH = pl.DeviceIdType.MESH
ND = 16
B = 160
GR = 4
RR = 40
SL = 8
STEPS = RR // SL
UNROLL = 8
LEAD = 2
SPLIT = (2, 4, 8, 8)
SWAP = 136


def to_tiles(block):
    rest = block.shape[2:]
    grouped = block.reshape((GR, RR, B) + rest)
    main = grouped[:, :, :128]
    rem = jnp.swapaxes(grouped[:, :, 128:], 0, 1).reshape((1, RR, 128) + rest)
    return jnp.concatenate([main, rem], axis=0)


def sigmoid(v):
    return 0.5 * jnp.tanh(0.5 * v) + 0.5


def norm_lanes(values, gamma, beta):
    centered = values - jnp.mean(values, axis=-1, keepdims=True)
    variance = jnp.mean(centered * centered, axis=-1, keepdims=True)
    return centered * lax.rsqrt(variance + NORM_EPS) * gamma + beta


def place(team):
    row, col = lax.axis_index('dap'), lax.axis_index('dap2')
    return row * 4 + col if team == ND else row * 2 + lax.rem(col, 2)


def partner(team, n):
    other = lax.rem(place(team) + n, team)
    if team == ND:
        return other, {'dap': other // 4, 'dap2': lax.rem(other, 4)}
    half = lax.axis_index('dap2') // 2
    return other, {'dap': other // 2, 'dap2': half * 2 + lax.rem(other, 2)}


def greet(team):
    barrier = pltpu.get_barrier_semaphore()

    def signal(n, carry):
        _, device = partner(team, n)
        pl.semaphore_signal(barrier, inc=1, device_id=device, device_id_type=MESH)
        return carry

    lax.fori_loop(1, team, signal, 0)


class Refs:
    pass


WHOLE = 3


def channel_groups(kind):
    each = 16 if kind == 'in' else 8
    sizes = [each // n for n in SPLIT]
    return tuple((sum(sizes[:n]), sizes[n]) for n in range(len(SPLIT)))


def group_bytes(ref, q):
    if q == 0:
        return ref.at[:, :, pl.ds(0, 4)]
    return ref.at[pl.ds(0, 2 * ref.shape[0] // SPLIT[q]), :, pl.ds(0, 1)]


def position_step(finish, project, natural_in, s, r):
    natural_out = not project
    z_ref = r.z_own if natural_in else r.z_in
    if finish:
        zo_ref = r.zo_own if natural_out else r.z_out
    if project:
        row, col = lax.axis_index('dap'), lax.axis_index('dap2')
        pairs = ((r.out_a, r.a_in), (r.out_b, r.b_in))

        def push(q, slab, grp):
            start, count = (0, 16 if project == 'in' else 8) if q is None else channel_groups(project)[q]
            sem = 0 if q is None else q
            rows = pl.ds(pl.multiple_of(slab * SL, SL), SL)
            for k, (src, dst) in enumerate(pairs):
                team = 8 if project == 'in' and k == 1 else ND
                split = 8 if project == 'in' else ND
                each = 128 // split
                lane = col if team == ND else lax.rem(col, 2)
                lanes = pl.ds(pl.multiple_of(lane * 128, 128), 128)
                there = dst.at[pl.ds(start, count), row, grp, rows, lanes]

                def part(index):
                    return src.at[slab, pl.ds(index * each + start, count), grp]

                def send(n, carry):
                    other, device = partner(team, n)
                    if team != split:
                        other = device['dap'] * 2 + lax.rem(device['dap2'], 2)
                    pltpu.make_async_remote_copy(
                        src_ref=part(other), dst_ref=there, send_sem=r.send_sem.at[k], recv_sem=r.recv_sem.at[k, sem],
                        device_id=device, device_id_type=MESH).start()
                    return carry

                lax.fori_loop(1, team, send, 0)
                pltpu.make_async_copy(part(place(split)), there, r.recv_sem.at[k, sem]).start()

    if natural_in:
        def load(n, carry):
            for g in range(GR):
                z_ref[g, n] = r.z_in[g, n, :128]
                z_ref[GR, n, g * 32:(g + 1) * 32] = r.z_in[g, n, 128:]
            return carry

        lax.fori_loop(0, SL, load, 0)

    def group(grp, carry):
        if finish:
            @pl.when(s == 0)
            def _():
                r.arrive(grp)

            total = jnp.zeros((SL, 128), F32)
            for cb in range(8):
                total += jnp.sum(r.tri(cb * 16, grp).astype(F32), axis=0)
            mean = (total * (1.0 / 128))[None]
            total = jnp.zeros((SL, 128), F32)
            for cb in range(8):
                centered = r.tri(cb * 16, grp).astype(F32) - mean
                total += jnp.sum(centered * centered, axis=0)
            scale = lax.rsqrt(total * (1.0 / 128) + NORM_EPS)[None]
            for cb in range(8):
                sl = slice(cb * 16, (cb + 1) * 16)
                y = (r.tri(cb * 16, grp).astype(F32) - mean) * scale * r.gout[0, 0, sl][:, None] + r.bout[0, 0, sl][:, None]
                r.y_buf[cb * 128:(cb + 1) * 128, :] = y.reshape(128, 128)

        def tile(n, inner):
            zf = z_ref[grp, n].astype(F32)
            if finish:
                x = norm_lanes(zf, r.gin[0, 0], r.bin[0, 0]).astype(BF16)
                gate = sigmoid(jnp.dot(x, r.wg[0, 0], preferred_element_type=F32))
                y = r.y_buf[pl.ds(n, 128, stride=SL), :].astype(BF16)
                update = lax.dot_general(y, r.wo[0, 0], (((0,), (0,)), ((), ())), preferred_element_type=F32)
                znew = (zf + gate * update).astype(BF16)
                zo_ref[grp, n] = znew
                zf = znew.astype(F32)
            if project:
                x = norm_lanes(zf, r.gnext[0, 0], r.bnext[0, 0]).astype(BF16)
                q = lax.dot_general(r.wp[0, 0], x, (((1,), (1,)), ((), ())), preferred_element_type=F32)
                m = r.mask[grp, pl.ds(n, 1), :]
                base = pl.multiple_of(n * SWAP, 8)
                r.sa[pl.ds(base, 128), :] = m * sigmoid(q[128:256]) * q[:128]
                r.sb[pl.ds(base, 128), :] = m * sigmoid(q[384:]) * q[256:384]
            return inner

        lax.fori_loop(0, SL, tile, 0, unroll=UNROLL)

        if project:
            def swap(cb, inner):
                for u in range(8):
                    c = cb * 8 + u
                    r.out_a[s, c, grp] = r.sa[pl.ds(c, SL, stride=SWAP), :].astype(BF16)
                    r.out_b[s, c, grp] = r.sb[pl.ds(c, SL, stride=SWAP), :].astype(BF16)
                return inner

            lax.fori_loop(0, 16, swap, 0)

            @pl.when(s == 0)
            def _():
                if not finish:
                    @pl.when(grp == 0)
                    def _():
                        pl.semaphore_wait(pltpu.get_barrier_semaphore(), ND - 1)

                push(None, s, grp)
        return carry

    lax.fori_loop(0, 5, group, 0)

    if finish and natural_out:
        def store(n, carry):
            for g in range(GR):
                r.z_out[g, n, :128] = zo_ref[g, n]
                r.z_out[g, n, 128:] = zo_ref[GR, n, g * 32:(g + 1) * 32]
            return carry

        lax.fori_loop(0, SL, store, 0)

    if project:
        @pl.when((s > 0) & (s < WHOLE))
        def _():
            push(None, s, slice(None))

        @pl.when(s >= WHOLE)
        def _():
            push(0, s, slice(None))

        @pl.when(s == STEPS - 1)
        def _():
            for q in range(1, len(channel_groups(project))):
                def later(slab, carry):
                    push(q, slab, slice(None))
                    return carry

                lax.fori_loop(WHOLE, STEPS, later, 0)


def channel_step(incoming, r, put_main, put_rem):
    cols = 2 if incoming else 4

    def rem_columns(ref):
        width = ref.shape[-1]
        packed = ref[0, :, B:, :].astype(F32).reshape(4 * RR, width).astype(BF16)
        return jnp.dot(packed, r.perm[:width], preferred_element_type=F32)

    def natural(wide, blk):
        return jnp.concatenate([wide[blk * RR:(blk + 1) * RR, g * 128:(g + 1) * 128] for g in range(GR)], axis=0)

    wide = rem_columns(r.a)
    for blk in range(4):
        r.amat[blk * B:(blk + 1) * B, :512] = r.a[0, blk, :B, :]
        r.amat[blk * B:(blk + 1) * B, 512:] = natural(wide, blk).astype(BF16)
    wide = rem_columns(r.b)
    for blk in range(4):
        last = natural(wide, blk).astype(BF16)
        if incoming:
            r.bmat[blk * B:(blk + 1) * B, :256] = r.b[0, blk, :B, :]
            r.bmat[blk * B:(blk + 1) * B, 256:] = last
        else:
            r.bmat[blk * 128:(blk + 1) * 128, :512] = r.b[0, blk, :128, :]
            r.bmat[512 + blk * 32:512 + (blk + 1) * 32, :512] = r.b[0, blk, 128:B, :]
            r.bmat[blk * 128:(blk + 1) * 128, 512:] = last[:128]
            r.bmat[512 + blk * 32:512 + (blk + 1) * 32, 512:] = last[128:]
    contract = 0 if incoming else 1
    r.tmat[...] = lax.dot_general(r.amat[...], r.bmat[...], (((contract,), (contract,)), ((), ())), preferred_element_type=F32)

    def rows_of(blk, lanes):
        if incoming:
            return jnp.concatenate([r.tmat[blk * 128:(blk + 1) * 128, lanes], r.tmat[512 + blk * 32:512 + (blk + 1) * 32, lanes]], axis=0)
        return r.tmat[blk * B:(blk + 1) * B, lanes]

    packed = []
    for blk in range(4):
        for j in range(cols):
            put_main(blk * cols + j, rows_of(blk, slice(j * 128, (j + 1) * 128)))
        rem = rows_of(blk, slice(cols * 128, cols * 128 + 128))
        packed.append(jnp.concatenate([rem[g * RR:(g + 1) * RR] for g in range(GR)], axis=1))
    wide = jnp.dot(jnp.concatenate(packed, axis=0).astype(BF16), r.perm[:, :cols * 128], preferred_element_type=F32)
    for blk in range(4):
        for j in range(cols):
            put_rem(blk * cols + j, wide[blk * RR:(blk + 1) * RR, j * 128:(j + 1) * 128])


def update_kernel(finish, project, natural_in, *refs):
    refs = list(refs)
    take = lambda: refs.pop(0)
    r = Refs()
    r.z_in = take()
    if finish:
        t_ref = take()
        r.gin, r.bin, r.wg, r.gout, r.bout, r.wo = [take() for _ in range(6)]
    if project:
        r.perm, r.mask, r.gnext, r.bnext, r.wp = [take() for _ in range(5)]
    if finish:
        r.z_out = take()
    if project:
        t_out, r.a_in, r.b_in = [take() for _ in range(3)]
    if natural_in:
        r.z_own = take()
    if finish:
        r.y_buf, t_own, send_t, recv_t = [take() for _ in range(4)]
        if not project:
            r.zo_own = take()
    if project:
        r.sa, r.sb, r.out_a, r.out_b, r.send_sem, r.recv_sem = [take() for _ in range(6)]
        r.amat, r.bmat, r.tmat, abuf, bbuf, fetch_sem = [take() for _ in range(6)]
    step = pl.program_id(0)

    team = 8 if finish == 'in' else ND
    each, me = 128 // team, place(team)

    def give(s, grp, sem):
        there = t_own.at[pl.ds(me * each, each), s, grp]

        def send(n, inner):
            other, device = partner(team, n)
            pltpu.make_async_remote_copy(
                src_ref=t_ref.at[:, other, s, grp], dst_ref=there, send_sem=send_t, recv_sem=recv_t.at[sem],
                device_id=device, device_id_type=MESH).start()
            return inner

        lax.fori_loop(1, team, send, 0)
        pltpu.make_async_copy(t_ref.at[:, me, s, grp], there, recv_t.at[sem]).start()

    @pl.when(step == 0)
    def _():
        met = ND if project else team
        greet(met)
        if finish:
            pl.semaphore_wait(pltpu.get_barrier_semaphore(), met - 1)

            def piece(grp, carry):
                give(0, grp, STEPS + grp)
                return carry

            def slab(s, carry):
                give(s, slice(None), s)
                return carry

            lax.fori_loop(0, 5, piece, 0)
            lax.fori_loop(1, LEAD if project else STEPS, slab, 0)

    @pl.when(step < STEPS)
    def _():
        if finish:
            @pl.when(step > 0)
            def _():
                landed = t_own.at[:, step]
                pltpu.make_async_copy(landed, landed, recv_t.at[step]).wait()

            def arrive(grp):
                landed = t_own.at[:, 0, grp]
                pltpu.make_async_copy(landed, landed, recv_t.at[STEPS + grp]).wait()

            r.arrive = arrive
            r.tri = lambda c0, grp: t_own[c0:c0 + 16, step, grp]
        position_step(finish, project, natural_in, step, r)
        if finish and project:
            @pl.when(step + LEAD < STEPS)
            def _():
                give(step + LEAD, slice(None), step + LEAD)

    if project:
        @pl.when(step >= STEPS)
        def _():
            c = step - STEPS
            each = 16 if project == 'in' else 8
            pairs = ((r.a_in, abuf), (r.b_in, bbuf))

            def fetch(chan):
                slot = lax.rem(chan, 2)
                for k, (src, buf) in enumerate(pairs):
                    for g in range(5):
                        pltpu.make_async_copy(src.at[chan, :, g], buf.at[slot, :, pl.ds(g * RR, RR)], fetch_sem.at[k, slot]).start()

            groups = channel_groups(project)
            for q, (start, count) in enumerate(groups):
                @pl.when(c == start)
                def _():
                    for k, (src, _) in enumerate(pairs):
                        landed = group_bytes(src, q)
                        pltpu.make_async_copy(landed, landed, r.recv_sem.at[k, q]).wait()
                    fetch(c)

            slot = lax.rem(c, 2)
            for k, (_, buf) in enumerate(pairs):
                pltpu.make_async_copy(buf.at[slot], buf.at[slot], fetch_sem.at[k, slot]).wait()
            last = functools.reduce(lambda x, y: x | y, [c == start + count - 1 for start, count in groups])

            @pl.when(jnp.logical_not(last))
            def _():
                fetch(c + 1)

            r.a, r.b = abuf.at[pl.ds(slot, 1)], bbuf.at[pl.ds(slot, 1)]

            def put_main(owner, v):
                tiles = v.reshape(GR, STEPS, SL, 128).astype(BF16)
                for s in range(STEPS):
                    t_out[0, owner, s, :GR] = tiles[:, s]

            def put_rem(owner, v):
                t_out[0, owner, :, GR] = v.reshape(STEPS, SL, 128).astype(BF16)

            channel_step(project == 'in', r, put_main, put_rem)

            @pl.when(c == each - 1)
            def _():
                for k, (src, dst) in enumerate(((r.out_a, r.a_in), (r.out_b, r.b_in))):
                    if project == 'out':
                        sent = src.at[:, pl.ds(0, 128 - 8)]
                    elif k == 0:
                        sent = dst.at[pl.ds(0, 15)]
                    else:
                        sent = src.at[:, pl.ds(0, 128 - 16)]
                    pltpu.make_async_copy(sent, sent, r.send_sem.at[k]).wait()

    if finish:
        @pl.when(step == STEPS - 1)
        def _():
            team = 8 if finish == 'in' else ND
            sent = t_own.at[pl.ds(0, 128 - 128 // team)]
            pltpu.make_async_copy(sent, sent, send_t).wait()


def update_call(z, t, at, after, params, collective_id):
    kind = lambda which: None if which is None else 'in' if which[1] else 'out'
    finish, project = kind(at), kind(after)
    natural_in = z.shape[0] == GR
    slab = lambda n: jnp.minimum(n, STEPS - 1)
    z_spec = pl.BlockSpec((5, SL, 128, 128), lambda n: (0, slab(n), 0, 0))
    n_spec = pl.BlockSpec((GR, SL, B, 128), lambda n: (0, slab(n), 0, 0))
    anywhere = pl.BlockSpec(memory_space=pl.ANY)

    def weight(name, which):
        arr = params[name]
        return arr, pl.BlockSpec((1, 1) + arr.shape[2:], lambda n: tuple(which) + (0,) * (arr.ndim - 2))

    ins, outs, scratch, steps = [(z, n_spec if natural_in else z_spec)], [], [], STEPS
    if natural_in:
        scratch.append(pltpu.VMEM((5, SL, 128, 128), BF16))
    if finish:
        ins.append((t, anywhere))
        ins += [weight(name, at) for name in ('gin', 'bin', 'wg', 'gout', 'bout', 'wo')]
        outs.append((jax.ShapeDtypeStruct((5, RR, 128, 128) if project else (GR, RR, B, 128), BF16), z_spec if project else n_spec))
        scratch += [pltpu.VMEM((128 * SL, 128), F32), pltpu.VMEM((128, STEPS, 5, SL, 128), BF16)]
        scratch += [pltpu.SemaphoreType.DMA, pltpu.SemaphoreType.DMA((STEPS + 5,))]
        if not project:
            scratch.append(pltpu.VMEM((5, SL, 128, 128), BF16))
    if project:
        ins.append((params['perm'], pl.BlockSpec((512, 512), lambda n: (0, 0))))
        ins.append((params['mask'], pl.BlockSpec((5, SL, 128), lambda n: (0, slab(n), 0))))
        ins += [weight(name, after) for name in ('gin', 'bin', 'wp')]
        each, owners, width = (8, 16, 512) if project == 'out' else (16, 8, 256)
        steps += each
        outs.append((jax.ShapeDtypeStruct((each, owners, STEPS, 5, SL, 128), BF16),
                     pl.BlockSpec((1, owners, STEPS, 5, SL, 128), lambda n: (jnp.maximum(n - STEPS, 0), 0, 0, 0, 0, 0))))
        outs += [(jax.ShapeDtypeStruct((each, 4, 5, RR, w), BF16), anywhere) for w in (512, width)]
        scratch += [pltpu.VMEM((SWAP * SL, 128), F32)] * 2
        scratch += [pltpu.VMEM((STEPS, 128, 5, SL, 128), BF16)] * 2
        scratch += [pltpu.SemaphoreType.DMA((2,)), pltpu.SemaphoreType.DMA((2, len(SPLIT)))]
        scratch += [pltpu.VMEM((640, 640), BF16), pltpu.VMEM((640, width + 128), BF16), pltpu.VMEM((640, width + 128), F32)]
        scratch += [pltpu.VMEM((2, 4, 200, w), BF16) for w in (512, width)] + [pltpu.SemaphoreType.DMA((2, 2))]
    name = '_'.join((['finish', finish] if finish else []) + (['start', project] if project else []))
    return pl.pallas_call(
        functools.partial(update_kernel, finish, project, natural_in), name=name, grid=(steps,),
        in_specs=[spec for _, spec in ins], out_specs=[spec for _, spec in outs], out_shape=[shape for shape, _ in outs],
        scratch_shapes=scratch, compiler_params=pltpu.CompilerParams(
            dimension_semantics=('arbitrary',), vmem_limit_bytes=60 * 2 ** 20, collective_id=collective_id, has_side_effects=True),
    )(*[v for v, _ in ins])


def solution(mesh):
    pair_spec = P(('data', 'dap'), 'dap2', None)
    mask_spec = P(('data', 'dap'), 'dap2')

    def local_fn(pair_act, pair_mask, in_gamma, in_beta, w_proj, w_gate, out_gamma, out_beta, w_out):
        mask = to_tiles(pair_mask.astype(F32))
        z = pair_act.reshape(GR, RR, B, 128)
        src = jnp.arange(512)
        perm = (((src % 128) // 32 * 128 + src // 128 * 32 + src % 32)[:, None] == jnp.arange(512)[None, :]).astype(BF16)
        rowed = lambda v: v[:, :, None, :]
        wide = lambda v: jnp.broadcast_to(v[..., None], v.shape + (128,))
        params = dict(
            perm=perm, mask=mask, gin=rowed(in_gamma), bin=rowed(in_beta), wp=jnp.swapaxes(w_proj, 2, 3), wg=w_gate,
            gout=wide(out_gamma), bout=wide(out_beta), wo=w_out)
        layers = in_gamma.shape[0]
        t, _, _ = update_call(z, None, None, (0, 0), params, 1)
        for layer in range(layers):
            z, t, _, _ = update_call(z, t, (layer, 0), (layer, 1), params, 2 if layer == 0 else 3)
            if layer + 1 < layers:
                z, t, _, _ = update_call(z, t, (layer, 1), (layer + 1, 0), params, 4)
            else:
                z, = update_call(z, t, (layer, 1), None, params, 5)
        return z.reshape(B, B, 128)

    return jax.shard_map(local_fn, mesh=mesh, in_specs=(pair_spec, mask_spec) + (P(),) * 7, out_specs=pair_spec, check_vma=False)
```
